512 devices in a mesh: own: 8 (over z_lo, core), dom: 64 (over y, z_hi, x).
Axes of the slice: x: 4, y: 8, z: 8 (z_hi: 2, z_lo: 4; z = z_hi * 4 + z_lo), core: 2. Of those that a mesh axis runs over, the one named last changes fastest.
Arguments:
- background: bfloat16 [1024, 6, 4096], P(('own', 'dom')), may hold values from -6 to 6
- storm_track: float32 [2, 5], replicated, may hold values from 0.02 to 1638.4, as said below
- need_tiles: int32 [512, 32], P(('own', 'dom')), may hold values from 0 to 1023, as said below
- node_cells: int32 [16384, 1024], P(('own', 'dom')), may hold values from 0 to 4030, as said below
- node_fracs: float32 [2, 16384, 1024], P(None, ('own', 'dom')), may hold values from 0 to 1
- slot_count: int32 [16384], P(('own', 'dom')), may hold values from 256 to 1024
- elevation: float32 [8, 2097152], P('own', 'dom'), may hold values from 0 to 2
- bed_level: float32 [8, 2097152], P('own', 'dom'), may hold values from -1 to 1.5
Outputs:
- forcing: bfloat16 [16384, 6, 1024], P(('own', 'dom'))
- surge_level: float32 [8, 2097152], P('own', 'dom')
The draws below stay inside these ranges and needn't reach their ends.
Inputs may be any that keep to these rules, and one draw needn't show every extreme that they name: `need_tiles`: entries k * 4 to (k + 1) * 4 - 1 of a row name tiles of band k (tiles k * 128 to (k + 1) * 128 - 1); within a row the numbers (tile % 128) // 2 are all different. `node_cells`: value // 64 and value % 64 are both at most 62. `storm_track`: row k: centre column and row in cells, pressure deficit, radius of maximum wind in cells, shape exponent; all positive.
All inputs are finite; a program needn't handle non-finite values.
Results may differ from the reference program's by a relative error of at most 0.0023.
The reference program's roundings to bfloat16 on the way count: a program that leaves them out, or rounds other values in their place, can miss the bound.
Values may be sent and summed in bfloat16 or wider, within the bound.
No kernel may reach another device: no remote copies, remote signals or barrier semaphores. Data moves between devices by JAX's collectives and lax.ppermute only.
A program may use at most 64 MiB of HBM per device.

```python
import jax
import jax.numpy as jnp
from jax import lax

TILE = 64
TCOLS = 32
TILES_DEV = 2
FIELDS = 6
K_B = 4
NPS = 1024
SWEEPS = 4
NEED = 32
BAND = 128
TILES = 1024
GRID_ROWS = 2048
GRID_COLS = 2048
SLOTS = 16384
CHAIN = 2097152
N_OWN = 8
N_DOM = 64
DEVICES = 512


def draw_storm_track(key, part):
    streams = jax.random.split(key, 5)
    centre_col = jax.random.uniform(streams[0], (2,), jnp.float32, 0.2, 0.8) * GRID_COLS
    centre_row = jax.random.uniform(streams[1], (2,), jnp.float32, 0.2, 0.8) * GRID_ROWS
    deficit = jax.random.uniform(streams[2], (2,), jnp.float32, 0.5, 1.5)
    max_radius = jax.random.uniform(streams[3], (2,), jnp.float32, 0.02, 0.06) * GRID_COLS
    exponent = jax.random.uniform(streams[4], (2,), jnp.float32, 1.0, 2.0)
    return jnp.stack([centre_col, centre_row, deficit, max_radius, exponent], axis=1)


def draw_need_tiles(key, part):
    streams = jax.random.split(key, DEVICES)

    def one_row(stream):
        first, second = jax.random.split(stream)
        holder_slots = jax.random.permutation(first, N_DOM)[:NEED].astype(jnp.int32)
        band_index = jnp.arange(NEED, dtype=jnp.int32) // K_B
        within_holder = jax.random.randint(second, (NEED,), 0, TILES_DEV, dtype=jnp.int32)
        return band_index * BAND + holder_slots * TILES_DEV + within_holder
    return jax.vmap(one_row)(streams).astype(jnp.int32)


def draw_node_cells(key, part):
    first, second = jax.random.split(key)
    row_first = jax.random.randint(first, (SLOTS, NPS), 0, TILE - 1, dtype=jnp.int32)
    col_first = jax.random.randint(second, (SLOTS, NPS), 0, TILE - 1, dtype=jnp.int32)
    return (row_first * TILE + col_first).astype(jnp.int32)


def plant(drawn, stream_key, least, top_value):
    dims = drawn.shape
    place = [jax.random.randint(jax.random.fold_in(stream_key, axis), (), 0, dims[axis]) for axis in range(len(dims))]
    drawn = drawn.at[tuple(place)].set(least)
    longest = dims.index(max(dims))
    place[longest] = (place[longest] + 1) % dims[longest]
    return drawn.at[tuple(place)].set(top_value)


def block_scale(rng, shape, shards, smallest, top_value):
    def one(dim, blocks):
        draws = jax.random.uniform(jax.random.fold_in(jax.random.fold_in(rng, 6), dim), (blocks,), jnp.float32, smallest / len(shards), top_value / len(shards))
        return jnp.repeat(jnp.exp(draws), shape[dim] // blocks).reshape((-1,) + (1,) * (len(shape) - dim - 1))

    loudness = one(*shards[0])
    for cut in shards[1:]:
        loudness = loudness * one(*cut)
    return loudness


def noise(key, shape, scale, reach, pieces=(), held_as=jnp.bfloat16):
    values = jax.random.normal(key, shape, jnp.float32) * scale
    if len(pieces) > 0:
        values = block_scale(key, shape, pieces, -0.22, 0.18) * values
    return jnp.clip(values, min=-reach, max=reach).astype(held_as)


def setup_inputs(seed: int = 0) -> dict:
    arg_keys = jax.random.split(jax.random.key(seed), 9)
    background = noise(arg_keys[0], (TILES, FIELDS, TILE * TILE), 1.0, 6.0, ((0, 512),))
    storm_track = draw_storm_track(jax.random.fold_in(arg_keys[8], 71), 0)
    need_tiles = draw_need_tiles(jax.random.fold_in(arg_keys[8], 71), 0)
    node_cells = draw_node_cells(jax.random.fold_in(arg_keys[8], 71), 0)
    node_fracs = jnp.clip(1.0 * jax.random.uniform(arg_keys[4], (2, SLOTS, NPS), jnp.float32) ** block_scale(arg_keys[4], (2, SLOTS, NPS), ((1, 512),), -0.2, 0.2), 0.0, 1.0)
    slot_count = plant(jax.random.randint(arg_keys[5], (SLOTS,), NPS // 4, NPS + 1), jax.random.fold_in(arg_keys[5], 1), NPS // 4, NPS).astype(jnp.int32)
    elevation = jnp.clip(2.0 * jax.random.uniform(arg_keys[6], (N_OWN, CHAIN), jnp.float32) ** block_scale(arg_keys[6], (N_OWN, CHAIN), ((0, 8), (1, 64)), -0.2, 0.2), 0.0, 2.0)
    bed_level = jnp.clip(-1.0 + 2.5 * jax.random.uniform(arg_keys[7], (N_OWN, CHAIN), jnp.float32) ** block_scale(arg_keys[7], (N_OWN, CHAIN), ((0, 8), (1, 64)), -0.2, 0.2), -1.0, 1.5)
    return dict(background=background, storm_track=storm_track, need_tiles=need_tiles, node_cells=node_cells, node_fracs=node_fracs, slot_count=slot_count, elevation=elevation, bed_level=bed_level)


KAPPA = 0.08

def holland(tile_index, background, storm_track):
    cell_index = jnp.arange(TILE * TILE, dtype=jnp.int32)
    cell_row = (cell_index // TILE).astype(jnp.float32)
    cell_col = (cell_index % TILE).astype(jnp.float32)
    tile_row = (tile_index // TCOLS).astype(jnp.float32)
    tile_col = (tile_index % TCOLS).astype(jnp.float32)
    north_cell = tile_row[:, None] * TILE + cell_row[None, :]
    east_cell = tile_col[:, None] * TILE + cell_col[None, :]
    fields = []
    for time_level in range(2):
        offset_x = east_cell - storm_track[time_level, 0]
        offset_y = north_cell - storm_track[time_level, 1]
        radius = jnp.sqrt(offset_x * offset_x + offset_y * offset_y + 1.0)
        radial_ratio = jnp.exp(storm_track[time_level, 4] * jnp.log(storm_track[time_level, 3] / radius))
        pressure_decay = jnp.exp(-radial_ratio)
        wind_speed = jnp.sqrt(storm_track[time_level, 4] * storm_track[time_level, 2] * radial_ratio * pressure_decay)
        fields.append(-wind_speed * offset_y / radius)
        fields.append(wind_speed * offset_x / radius)
        fields.append(-storm_track[time_level, 2] * (1.0 - pressure_decay))
    return (background.astype(jnp.float32) + jnp.stack(fields, axis=1)).astype(jnp.bfloat16)

def interpolate(tile_data, cell_index, fractions, counts):
    flat = tile_data.astype(jnp.float32)

    def corner(offset):
        index = (cell_index + offset).astype(jnp.int32)
        return jnp.take_along_axis(flat, index[:, None, :], axis=2)
    near_weight = lax.optimization_barrier((1.0 - fractions[0]).astype(jnp.bfloat16)).astype(jnp.float32)
    far_weight = lax.optimization_barrier(fractions[0].astype(jnp.bfloat16)).astype(jnp.float32)
    upper_row = corner(0) * near_weight[:, None, :] + corner(1) * far_weight[:, None, :]
    bottom = corner(TILE) * near_weight[:, None, :] + corner(TILE + 1) * far_weight[:, None, :]
    north_frac = fractions[1][:, None, :]
    node_value = (1.0 - north_frac) * upper_row + north_frac * bottom
    live = jnp.arange(NPS, dtype=jnp.int32)[None, :] < counts[:, None]
    return jnp.where(live[:, None, :], node_value, jnp.float32(0.0))

def flux_sweep(elevation, bed_level):
    surface = elevation
    for sweep_step in range(SWEEPS):
        wet_depth = jnp.maximum(surface - bed_level, 0.0)
        slope_drop = surface[:, :-1] - surface[:, 1:]
        upwind = jnp.where(slope_drop >= 0.0, wet_depth[:, :-1], wet_depth[:, 1:])
        face_flux = KAPPA * upwind * slope_drop
        wall_zero = jnp.zeros((surface.shape[0], 1), jnp.float32)
        faces = jnp.concatenate([wall_zero, face_flux, wall_zero], axis=1)
        surface = surface - (faces[:, 1:] - faces[:, :-1])
    return surface

def reference(background, storm_track, need_tiles, node_cells, node_fracs, slot_count, elevation, bed_level):
    forcing_grid = holland(jnp.arange(TILES, dtype=jnp.int32), background, storm_track)
    cell_parts = node_cells.reshape(DEVICES, NEED, NPS)
    frac_parts = jnp.moveaxis(node_fracs.reshape(2, DEVICES, NEED, NPS), 1, 0)
    count_parts = slot_count.reshape(DEVICES, NEED)

    def device_part(packed):
        wanted, cell_part, frac_part, count_part = packed
        return interpolate(jnp.take(forcing_grid, wanted.astype(jnp.int32), axis=0), cell_part, frac_part, count_part)
    values = lax.map(device_part, (need_tiles, cell_parts, frac_parts, count_parts))
    forcing = values.reshape(SLOTS, FIELDS, NPS).astype(jnp.bfloat16)
    pressure = values[:, :, 5, :].reshape(N_OWN, CHAIN)
    surface = flux_sweep(elevation, bed_level)
    surge_level = surface - 0.5 * pressure * jnp.clip(surface - bed_level, 0.0, 1.0)
    return (forcing, surge_level)
```

```python
import jax
import jax.numpy as jnp
from jax import lax
from jax.experimental import pallas as pl
from jax.experimental.pallas import tpu as pltpu
from jax.sharding import PartitionSpec as P

TILE = 64
TCOLS = 32
TILES_DEV = 2
FIELDS = 6
SWEEPS = 4
KAPPA = 0.08
NEED = 32
NPS = 1024
LANES = 128
GROUPS = NPS // LANES
N_OWN = 8
N_DOM = 64
BAND = TILES_DEV * N_DOM
CORES = 2
MSG = 16
DEAD_CELL = 0xFFC0
EDGE_SCALE = 2.0**29
FX_STEP = 2.0**-16
FY_TOP = 65535.0


SMALL = pltpu.CompilerParams(vmem_limit_bytes=8 * 2**20)


def iota(shape, dim):
    return lax.broadcasted_iota(jnp.int32, shape, dim)


def holland_kernel(place_ref, track_ref, background_ref, out_ref, rows_ref):
    field = iota((8, LANES), 0)
    lane = iota((8, LANES), 1)
    late = field >= 3
    centre_x, centre_y, deficit, max_radius, exponent = (
        jnp.where(late, track_ref[1, i], track_ref[0, i]) for i in range(5)
    )
    kind = jnp.where(late, field - 3, field)
    strength = exponent * deficit
    left = lane < TILE

    def one_field(tile, chunk):
        tile_index = place_ref[0] * TILES_DEV + tile
        north = (tile_index // TCOLS * TILE + 2 * chunk + lane // TILE).astype(jnp.float32)
        east = (tile_index % TCOLS * TILE + lane % TILE).astype(jnp.float32)
        offset_x = east - centre_x
        offset_y = north - centre_y
        radius = jnp.sqrt(offset_x * offset_x + offset_y * offset_y + 1.0)
        ratio = jnp.exp(exponent * jnp.log(max_radius / radius))
        decay = jnp.exp(-ratio)
        speed = jnp.sqrt(strength * ratio * decay)
        wind = speed * jnp.where(kind == 0, -offset_y, offset_x) / radius
        storm = jnp.where(kind == 2, -deficit * (1.0 - decay), wind)
        piece = background_ref[tile, :, pl.ds(pl.multiple_of(chunk * LANES, LANES), LANES)]
        return piece.astype(jnp.float32) + storm[:FIELDS]

    def step(chunk, carry):
        first = one_field(0, chunk)
        second = one_field(1, chunk)
        even = jnp.where(left[:FIELDS], first, pltpu.roll(second, TILE, 1))
        odd = jnp.where(left[:FIELDS], pltpu.roll(first, TILE, 1), second)
        rows_ref[pl.ds(2 * chunk, FIELDS, stride=TILE), :] = even
        rows_ref[pl.ds(2 * chunk + 1, FIELDS, stride=TILE), :] = odd
        return carry

    lax.fori_loop(0, TILE // 2, step, 0)
    out_ref[...] = rows_ref[...].astype(jnp.bfloat16)


def holland(place, storm_track, background):
    rows = FIELDS * TILE
    return pl.pallas_call(
        holland_kernel,
        out_shape=jax.ShapeDtypeStruct((rows, LANES), jnp.bfloat16),
        in_specs=[
            pl.BlockSpec(memory_space=pltpu.SMEM),
            pl.BlockSpec(memory_space=pltpu.SMEM),
            pl.BlockSpec(memory_space=pltpu.VMEM),
        ],
        out_specs=pl.BlockSpec(memory_space=pltpu.VMEM),
        scratch_shapes=[pltpu.VMEM((rows, LANES), jnp.float32)],
        compiler_params=SMALL,
    )(place, storm_track, background)


def column_code(fraction):
    scaled = fraction * 32768.0
    whole = jnp.floor(scaled)
    code = 2.0 * whole + jnp.where(scaled > whole, 1.0, 0.0)
    return jnp.minimum(code, 65535.0).astype(jnp.int32)


def row_code(fraction):
    return jnp.floor(fraction * FY_TOP + 0.5).astype(jnp.int32)


def edge_code(value):
    return jnp.floor(value * EDGE_SCALE + 0.5).astype(jnp.int32)


def query_kernel(
    need_ref, count_ref, cells_ref, fracs_ref, ehead_ref, etail_ref, bhead_ref, btail_ref, out_ref, stage_ref
):
    for g in range(GROUPS):
        span = slice(g * LANES, (g + 1) * LANES)
        word = cells_ref[:, span] | (column_code(fracs_ref[0, :, span]) << 16)
        stage_ref[pl.ds(g, NEED, stride=MSG), :] = word
    for g in range(GROUPS // 2):
        low = row_code(fracs_ref[1, :, g * LANES : (g + 1) * LANES])
        high = row_code(fracs_ref[1, :, NPS // 2 + g * LANES : NPS // 2 + (g + 1) * LANES])
        stage_ref[pl.ds(GROUPS + g, NEED, stride=MSG), :] = low | (high << 16)
    row = iota((8, LANES), 0)
    lane = iota((8, LANES), 1)
    position = row * LANES + lane
    surface = jnp.where(lane < SWEEPS, ehead_ref[0:1, :], etail_ref[7:8, :])
    bed = jnp.where(lane < SWEEPS, bhead_ref[0:1, :], btail_ref[7:8, :])
    plain = jnp.where(row == 5, edge_code(surface), jnp.where(row == 6, edge_code(bed), -1))

    def clear(d, carry):
        out_ref[d, 8:16, :] = plain
        return carry

    lax.fori_loop(0, N_DOM, clear, 0, unroll=8)

    def place(s, carry):
        tile = need_ref[0, s]
        count = count_ref[s]
        holder = tile % BAND // TILES_DEV
        header = (tile // BAND * TILES_DEV + tile % TILES_DEV) | (count << 16)
        start = pl.multiple_of(s * MSG, MSG)
        out_ref[holder, 0:8, :] = jnp.where(position < count, stage_ref[pl.ds(start, 8), :], DEAD_CELL)
        out_ref[holder, 8:16, :] = jnp.where(
            row < 4, stage_ref[pl.ds(start + 8, 8), :], jnp.where(row == 4, header, plain)
        )
        return carry

    lax.fori_loop(0, NEED, place, 0, unroll=4)


def queries(need_tiles, slot_count, node_cells, node_fracs, elevation, bed_level):
    last = elevation.shape[0] // 8 - 1
    head = pl.BlockSpec((8, LANES), lambda i: (0, 0))
    tail = pl.BlockSpec((8, LANES), lambda i: (last, 0))
    return pl.pallas_call(
        query_kernel,
        grid=(1,),
        out_shape=jax.ShapeDtypeStruct((N_DOM, MSG, LANES), jnp.int32),
        in_specs=[
            pl.BlockSpec(memory_space=pltpu.SMEM),
            pl.BlockSpec(memory_space=pltpu.SMEM),
            pl.BlockSpec(memory_space=pltpu.VMEM),
            pl.BlockSpec(memory_space=pltpu.VMEM),
            head,
            tail,
            head,
            tail,
        ],
        out_specs=pl.BlockSpec(memory_space=pltpu.VMEM),
        scratch_shapes=[pltpu.VMEM((NEED * MSG, LANES), jnp.int32)],
        compiler_params=SMALL,
    )(need_tiles, slot_count, node_cells, node_fracs, elevation, elevation, bed_level, bed_level)


CHUNK = 256


def interpolate_kernel(
    place_ref, header_ref, message_ref, near0, near1, near2, near3, far_ref, out_ref, tiles_ref, x_ref, y_ref, part_ref
):
    own = place_ref[0]
    for shift, ref in enumerate((near0, near1, near2, near3)):
        band = (own + N_OWN - CORES * shift) % N_OWN
        tiles_ref[2 * band] = ref[:, 0:TILE]
        tiles_ref[2 * band + 1] = ref[:, TILE : 2 * TILE]
        band = band + 1 - 2 * (band % CORES)
        tiles_ref[2 * band] = far_ref[shift, :, 0:TILE]
        tiles_ref[2 * band + 1] = far_ref[shift, :, TILE : 2 * TILE]
    spot = iota((TILE, CHUNK), 0).astype(jnp.float32)
    per_chunk = CHUNK // LANES

    def one_slot(s, carry):
        header = header_ref[s]

        @pl.when(header >= 0)
        def _():
            count = header >> 16
            word = message_ref[s, 0:8, :]
            cell = word & 0xFFFF
            x_ref[...] = (cell & (TILE - 1)).astype(jnp.float32) + lax.shift_right_logical(word, 16).astype(
                jnp.float32
            ) * FX_STEP
            pair = message_ref[s, 8:16, :]
            row = (cell // TILE).astype(jnp.float32)
            y_ref[0:4, :] = row[0:4] + (pair[0:4] & 0xFFFF).astype(jnp.float32) * (1.0 / FY_TOP)
            y_ref[4:8, :] = row[4:8] + lax.shift_right_logical(pair[0:4], 16).astype(jnp.float32) * (1.0 / FY_TOP)
            tile = tiles_ref[header & 0xFFFF]
            for c in range(NPS // CHUNK):

                @pl.when(c * CHUNK < count)
                def _():
                    g = c * per_chunk
                    x = jnp.concatenate([x_ref[g + i : g + i + 1, :] for i in range(per_chunk)], axis=1)
                    y = jnp.concatenate([y_ref[g + i : g + i + 1, :] for i in range(per_chunk)], axis=1)
                    columns = jnp.maximum(1.0 - jnp.abs(spot - x), 0.0).astype(jnp.bfloat16)
                    rows = jnp.maximum(1.0 - jnp.abs(spot - y), 0.0)
                    spread = jnp.dot(tile, columns, preferred_element_type=jnp.float32)
                    for f in range(FIELDS):
                        weighed = (spread[f * TILE : (f + 1) * TILE] * rows).reshape(TILE // 8, 8, CHUNK)
                        total = jnp.sum(weighed, axis=0)
                        for i in range(per_chunk):
                            at = (f * GROUPS + g + i) * 8
                            part_ref[at : at + 8, :] = total[:, i * LANES : (i + 1) * LANES]

                @pl.when(c * CHUNK >= count)
                def _():
                    for f in range(FIELDS):
                        at = (f * GROUPS + c * per_chunk) * 8
                        part_ref[at : at + 8 * per_chunk, :] = jnp.zeros((8 * per_chunk, LANES), jnp.float32)

            values = []
            for f in range(FIELDS):
                value = part_ref[pl.ds(f * 64, GROUPS, stride=8), :]
                for i in range(1, 8):
                    value = value + part_ref[pl.ds(f * 64 + i, GROUPS, stride=8), :]
                values.append(value)
            out_ref[s] = jnp.concatenate(values, axis=0).astype(jnp.bfloat16)

        return carry

    lax.fori_loop(0, N_DOM, one_slot, 0)


def interpolate(place, header, message, near, far):
    return pl.pallas_call(
        interpolate_kernel,
        out_shape=jax.ShapeDtypeStruct((N_DOM, FIELDS * GROUPS, LANES), jnp.bfloat16),
        in_specs=[pl.BlockSpec(memory_space=pltpu.SMEM)] * 2 + [pl.BlockSpec(memory_space=pltpu.VMEM)] * 6,
        out_specs=pl.BlockSpec(memory_space=pltpu.VMEM),
        scratch_shapes=[
            pltpu.VMEM((N_OWN * TILES_DEV, FIELDS * TILE, TILE), jnp.bfloat16),
            pltpu.VMEM((GROUPS, LANES), jnp.float32),
            pltpu.VMEM((GROUPS, LANES), jnp.float32),
            pltpu.VMEM((FIELDS * GROUPS * 8, LANES), jnp.float32),
        ],
        compiler_params=SMALL,
    )(place, header, message, *near, far)


def following(x, lane):
    moved = pltpu.roll(x, LANES - 1, 1)
    return jnp.where(lane == LANES - 1, pltpu.roll(moved, x.shape[0] - 1, 0), moved)


def preceding(x, lane):
    moved = pltpu.roll(x, 1, 1)
    return jnp.where(lane == 0, pltpu.roll(moved, 1, 0), moved)


def flux_kernel(place_ref, before_ref, after_ref, elevation_ref, bed_ref, out_ref):
    rows = elevation_ref.shape[0]
    lane8 = iota((8, LANES), 1)
    row8 = iota((8, LANES), 0)

    def ends(which):
        before = before_ref[0, which : which + 1, :].astype(jnp.float32) * (1.0 / EDGE_SCALE)
        after = after_ref[0, which : which + 1, :].astype(jnp.float32) * (1.0 / EDGE_SCALE)
        top = jnp.where((row8 == 7) & (lane8 >= LANES - SWEEPS), before, 0.0)
        bottom = jnp.where((row8 == 0) & (lane8 < SWEEPS), after, 0.0)
        return top, bottom

    surface_top, surface_bottom = ends(5)
    bed_top, bed_bottom = ends(6)
    surface = jnp.concatenate([surface_top, elevation_ref[...], surface_bottom], axis=0)
    bed = jnp.concatenate([bed_top, bed_ref[...], bed_bottom], axis=0)
    lane = iota(surface.shape, 1)
    node = iota(surface.shape, 0) * LANES + lane
    first_wall = jnp.where(place_ref[2] == 0, 8 * LANES - 1, -1)
    last_wall = jnp.where(place_ref[2] == N_DOM - 1, (8 + rows) * LANES - 1, -1)
    open_face = jnp.where((node == first_wall) | (node == last_wall), 0.0, KAPPA)
    for sweep_step in range(SWEEPS):
        wet = jnp.maximum(surface - bed, 0.0)
        drop = surface - following(surface, lane)
        upwind = jnp.where(drop >= 0.0, wet, following(wet, lane))
        flux = open_face * upwind * drop
        surface = surface - (flux - preceding(flux, lane))
    out_ref[...] = surface[8 : 8 + rows]


def flux_sweeps(place, message, elevation, bed_level):
    whole = pl.BlockSpec(elevation.shape, lambda i, place_ref: (0, 0))
    return pl.pallas_call(
        flux_kernel,
        out_shape=jax.ShapeDtypeStruct(elevation.shape, jnp.float32),
        grid_spec=pltpu.PrefetchScalarGridSpec(
            num_scalar_prefetch=1,
            grid=(1,),
            in_specs=[
                pl.BlockSpec((1, 8, LANES), lambda i, place_ref: (place_ref[0], 1, 0)),
                pl.BlockSpec((1, 8, LANES), lambda i, place_ref: (place_ref[1], 1, 0)),
                whole,
                whole,
            ],
            out_specs=whole,
        ),
        compiler_params=SMALL,
    )(place, message, message, elevation, bed_level)


SLOTS8 = 8


def finish_kernel(need_ref, returned_ref, surface_ref, bed_ref, forcing_ref, surge_ref, stage_ref):
    rows = FIELDS * GROUPS

    def eight_slots(b, carry):
        for i in range(SLOTS8):
            s = b * SLOTS8 + i
            block = returned_ref[need_ref[0, s] % BAND // TILES_DEV].astype(jnp.float32)
            stage_ref[i * rows : (i + 1) * rows, :] = block
            here = pl.ds(pl.multiple_of(s * GROUPS, GROUPS), GROUPS)
            surface = surface_ref[here, :]
            wet = jnp.minimum(jnp.maximum(surface - bed_ref[here, :], 0.0), 1.0)
            surge_ref[here, :] = surface - 0.5 * block[rows - GROUPS :] * wet
        slots = pl.ds(pl.multiple_of(b * SLOTS8, SLOTS8), SLOTS8)
        for f in range(FIELDS):
            for g in range(GROUPS):
                piece = stage_ref[pl.ds(f * GROUPS + g, SLOTS8, stride=rows), :]
                forcing_ref[f, slots, g * LANES : (g + 1) * LANES] = piece.astype(jnp.bfloat16)
        return carry

    lax.fori_loop(0, NEED // SLOTS8, eight_slots, 0)


def finish(need_tiles, returned, surface, bed_level):
    vmem = pl.BlockSpec(memory_space=pltpu.VMEM)
    return pl.pallas_call(
        finish_kernel,
        out_shape=(
            jax.ShapeDtypeStruct((FIELDS, NEED, NPS), jnp.bfloat16),
            jax.ShapeDtypeStruct(surface.shape, jnp.float32),
        ),
        in_specs=[pl.BlockSpec(memory_space=pltpu.SMEM), vmem, vmem, vmem],
        out_specs=(vmem, vmem),
        scratch_shapes=[pltpu.VMEM((SLOTS8 * FIELDS * GROUPS, LANES), jnp.float32)],
        compiler_params=SMALL,
    )(need_tiles, returned, surface, bed_level)


def exchange(blocks, axis):
    return lax.all_to_all(blocks, axis, split_axis=0, concat_axis=0, tiled=True)


def shards(
    background, storm_track, need_tiles, node_cells, node_fracs, slot_count, elevation, bed_level
):
    own = lax.axis_index("own")
    dom = lax.axis_index("dom")
    elevation = elevation.reshape(-1, LANES)
    bed_level = bed_level.reshape(-1, LANES)
    tiles = holland((own * N_DOM + dom)[None].astype(jnp.int32), storm_track, background)
    near = [tiles]
    for shift in range(CORES, N_OWN, CORES):
        near.append(lax.ppermute(tiles, "own", [(i, (i + shift) % N_OWN) for i in range(N_OWN)]))
    far = lax.ppermute(jnp.stack(near), "own", [(i, i ^ 1) for i in range(N_OWN)])
    question = queries(need_tiles, slot_count, node_cells, node_fracs, elevation, bed_level)
    message = exchange(question, "dom")
    answers = interpolate(own[None].astype(jnp.int32), message[:, 12, 0], message, near, far)
    returned = exchange(answers, "dom")
    place = jnp.stack([(dom - 1) % N_DOM, (dom + 1) % N_DOM, dom]).astype(jnp.int32)
    surface = flux_sweeps(place, message, elevation, bed_level)
    forcing, surge = finish(need_tiles, returned, surface, bed_level)
    return forcing.transpose(1, 0, 2), surge.reshape(1, -1)


def solution(mesh):
    placed = (
        P(("own", "dom"), None, None),
        P(),
        P(("own", "dom"), None),
        P(("own", "dom"), None),
        P(None, ("own", "dom"), None),
        P(("own", "dom")),
        P("own", "dom"),
        P("own", "dom"),
    )
    return jax.shard_map(
        shards,
        mesh=mesh,
        in_specs=placed,
        out_specs=(P(("own", "dom"), None, None), P("own", "dom")),
        check_vma=False,
    )
```

```python
import jax
import jax.numpy as jnp
from jax import lax
from jax.experimental import pallas as pl
from jax.experimental.pallas import tpu as pltpu
from jax.sharding import PartitionSpec as P

TILE = 64
TCOLS = 32
TILES_DEV = 2
FIELDS = 6
SWEEPS = 4
KAPPA = 0.08
NEED = 32
NPS = 1024
LANES = 128
GROUPS = NPS // LANES
N_OWN = 8
N_DOM = 64
BAND = TILES_DEV * N_DOM
MSG = 16
DEAD_CELL = 0xFFC0
EDGE_SCALE = 2.0**29
FX_STEP = 2.0**-16
FY_TOP = 65535.0


SMALL = pltpu.CompilerParams(vmem_limit_bytes=8 * 2**20)


def iota(shape, dim):
    return lax.broadcasted_iota(jnp.int32, shape, dim)


def holland_kernel(place_ref, track_ref, background_ref, out_ref, rows_ref):
    field = iota((8, LANES), 0)
    lane = iota((8, LANES), 1)
    late = field >= 3
    centre_x, centre_y, deficit, max_radius, exponent = (
        jnp.where(late, track_ref[1, i], track_ref[0, i]) for i in range(5)
    )
    kind = jnp.where(late, field - 3, field)
    strength = exponent * deficit
    left = lane < TILE

    def one_field(tile, chunk):
        tile_index = place_ref[0] * TILES_DEV + tile
        north = (tile_index // TCOLS * TILE + 2 * chunk + lane // TILE).astype(jnp.float32)
        east = (tile_index % TCOLS * TILE + lane % TILE).astype(jnp.float32)
        offset_x = east - centre_x
        offset_y = north - centre_y
        radius = jnp.sqrt(offset_x * offset_x + offset_y * offset_y + 1.0)
        ratio = jnp.exp(exponent * jnp.log(max_radius / radius))
        decay = jnp.exp(-ratio)
        speed = jnp.sqrt(strength * ratio * decay)
        wind = speed * jnp.where(kind == 0, -offset_y, offset_x) / radius
        storm = jnp.where(kind == 2, -deficit * (1.0 - decay), wind)
        piece = background_ref[tile, :, pl.ds(pl.multiple_of(chunk * LANES, LANES), LANES)]
        return piece.astype(jnp.float32) + storm[:FIELDS]

    def step(chunk, carry):
        first = one_field(0, chunk)
        second = one_field(1, chunk)
        even = jnp.where(left[:FIELDS], first, pltpu.roll(second, TILE, 1))
        odd = jnp.where(left[:FIELDS], pltpu.roll(first, TILE, 1), second)
        rows_ref[pl.ds(2 * chunk, FIELDS, stride=TILE), :] = even
        rows_ref[pl.ds(2 * chunk + 1, FIELDS, stride=TILE), :] = odd
        return carry

    lax.fori_loop(0, TILE // 2, step, 0, unroll=4)
    out_ref[...] = rows_ref[...].astype(jnp.bfloat16)


def holland(place, storm_track, background):
    rows = FIELDS * TILE
    return pl.pallas_call(
        holland_kernel,
        out_shape=jax.ShapeDtypeStruct((rows, LANES), jnp.bfloat16),
        in_specs=[
            pl.BlockSpec(memory_space=pltpu.SMEM),
            pl.BlockSpec(memory_space=pltpu.SMEM),
            pl.BlockSpec(memory_space=pltpu.VMEM),
        ],
        out_specs=pl.BlockSpec(memory_space=pltpu.VMEM),
        scratch_shapes=[pltpu.VMEM((rows, LANES), jnp.float32)],
        compiler_params=SMALL,
    )(place, storm_track, background)


def column_code(fraction):
    scaled = fraction * 32768.0
    whole = jnp.floor(scaled)
    code = 2.0 * whole + jnp.where(scaled > whole, 1.0, 0.0)
    return jnp.minimum(code, 65535.0).astype(jnp.int32)


def row_code(fraction):
    return jnp.floor(fraction * FY_TOP + 0.5).astype(jnp.int32)


def edge_code(value):
    return jnp.floor(value * EDGE_SCALE + 0.5).astype(jnp.int32)


def query_kernel(
    need_ref, count_ref, cells_ref, fracs_ref, ehead_ref, etail_ref, bhead_ref, btail_ref, out_ref, stage_ref
):
    for g in range(GROUPS):
        span = slice(g * LANES, (g + 1) * LANES)
        word = cells_ref[:, span] | (column_code(fracs_ref[0, :, span]) << 16)
        stage_ref[pl.ds(g, NEED, stride=MSG), :] = word
    for g in range(GROUPS // 2):
        low = row_code(fracs_ref[1, :, g * LANES : (g + 1) * LANES])
        high = row_code(fracs_ref[1, :, NPS // 2 + g * LANES : NPS // 2 + (g + 1) * LANES])
        stage_ref[pl.ds(GROUPS + g, NEED, stride=MSG), :] = low | (high << 16)
    row = iota((8, LANES), 0)
    lane = iota((8, LANES), 1)
    position = row * LANES + lane
    surface = jnp.where(lane < SWEEPS, ehead_ref[0:1, :], etail_ref[7:8, :])
    bed = jnp.where(lane < SWEEPS, bhead_ref[0:1, :], btail_ref[7:8, :])
    plain = jnp.where(row == 5, edge_code(surface), jnp.where(row == 6, edge_code(bed), -1))

    def clear(d, carry):
        out_ref[d, 8:16, :] = plain
        return carry

    lax.fori_loop(0, N_DOM, clear, 0, unroll=8)

    def place(s, carry):
        tile = need_ref[0, s]
        count = count_ref[s]
        holder = tile % BAND // TILES_DEV
        header = (tile // BAND * TILES_DEV + tile % TILES_DEV) | (count << 16)
        start = pl.multiple_of(s * MSG, MSG)
        out_ref[holder, 0:8, :] = jnp.where(position < count, stage_ref[pl.ds(start, 8), :], DEAD_CELL)
        out_ref[holder, 8:16, :] = jnp.where(
            row < 4, stage_ref[pl.ds(start + 8, 8), :], jnp.where(row == 4, header, plain)
        )
        return carry

    lax.fori_loop(0, NEED, place, 0, unroll=4)


def queries(need_tiles, slot_count, node_cells, node_fracs, elevation, bed_level):
    last = elevation.shape[0] // 8 - 1
    head = pl.BlockSpec((8, LANES), lambda i: (0, 0))
    tail = pl.BlockSpec((8, LANES), lambda i: (last, 0))
    return pl.pallas_call(
        query_kernel,
        grid=(1,),
        out_shape=jax.ShapeDtypeStruct((N_DOM, MSG, LANES), jnp.int32),
        in_specs=[
            pl.BlockSpec(memory_space=pltpu.SMEM),
            pl.BlockSpec(memory_space=pltpu.SMEM),
            pl.BlockSpec(memory_space=pltpu.VMEM),
            pl.BlockSpec(memory_space=pltpu.VMEM),
            head,
            tail,
            head,
            tail,
        ],
        out_specs=pl.BlockSpec(memory_space=pltpu.VMEM),
        scratch_shapes=[pltpu.VMEM((NEED * MSG, LANES), jnp.int32)],
    )(need_tiles, slot_count, node_cells, node_fracs, elevation, elevation, bed_level, bed_level)


CHUNK = 256
PER_CHUNK = CHUNK // LANES
CHUNKS = NPS // CHUNK


def interpolate_kernel(header_ref, message_ref, column_ref, out_ref, tiles_ref, x_ref, y_ref, part_ref):
    for k in range(N_OWN):
        tiles_ref[2 * k] = column_ref[k, :, 0:TILE]
        tiles_ref[2 * k + 1] = column_ref[k, :, TILE : 2 * TILE]
    spot = iota((TILE, LANES), 0).astype(jnp.float32)

    def add_up(slot):
        values = []
        for f in range(FIELDS):
            pieces = [part_ref[pl.ds(f * 64 + i, GROUPS, stride=8), :] for i in range(8)]
            while len(pieces) > 1:
                pieces = [a + b for a, b in zip(pieces[::2], pieces[1::2])]
            values.append(pieces[0])
        out_ref[slot] = jnp.concatenate(values, axis=0).astype(jnp.bfloat16)

    def hat(ref, g):
        return jnp.maximum(1.0 - jnp.abs(spot - ref[g : g + 1, :]), 0.0)

    def one_slot(s, header, before, live):
        add_up(before)
        word = message_ref[s, 0:8, :]
        pair = message_ref[s, 8:16, :]
        cell = word & 0xFFFF
        row = (cell // TILE).astype(jnp.float32)
        low = (pair[0:4] & 0xFFFF).astype(jnp.float32)
        high = lax.shift_right_logical(pair[0:4], 16).astype(jnp.float32)
        x_ref[...] = (cell & (TILE - 1)).astype(jnp.float32) + lax.shift_right_logical(word, 16).astype(
            jnp.float32
        ) * FX_STEP
        y_ref[0:4, :] = row[0:4] + low * (1.0 / FY_TOP)
        y_ref[4:8, :] = row[4:8] + high * (1.0 / FY_TOP)
        tile = tiles_ref[header & 0xFFFF]
        for c in range(live):
            g = c * PER_CHUNK
            groups = range(g, g + PER_CHUNK)
            columns = jnp.concatenate([hat(x_ref, i).astype(jnp.bfloat16) for i in groups], axis=1)
            spread = jnp.dot(tile, columns, preferred_element_type=jnp.float32)
            for i in groups:
                rows = hat(y_ref, i)
                lanes = slice((i - g) * LANES, (i - g + 1) * LANES)
                for f in range(FIELDS):
                    weighed = (spread[f * TILE : (f + 1) * TILE, lanes] * rows).reshape(TILE // 8, 8, LANES)
                    at = (f * GROUPS + i) * 8
                    part_ref[at : at + 8, :] = jnp.sum(weighed, axis=0)
        dead = (CHUNKS - live) * PER_CHUNK * 8
        if dead:
            for f in range(FIELDS):
                at = (f + 1) * GROUPS * 8 - dead
                part_ref[at : at + dead, :] = jnp.zeros((dead, LANES), jnp.float32)

    def step(s, last):
        header = header_ref[s]
        live = jnp.maximum(((header >> 16) + CHUNK - 1) // CHUNK, 2)
        before = jnp.where(last < 0, s, last)
        for m in range(2, CHUNKS + 1):

            @pl.when((header >= 0) & (live == m))
            def _():
                one_slot(s, header, before, m)

        return jnp.where(header >= 0, s, last)

    last = lax.fori_loop(0, N_DOM, step, -1)
    add_up(jnp.maximum(last, 0))


def interpolate(header, message, column):
    return pl.pallas_call(
        interpolate_kernel,
        out_shape=jax.ShapeDtypeStruct((N_DOM, FIELDS * GROUPS, LANES), jnp.bfloat16),
        in_specs=[pl.BlockSpec(memory_space=pltpu.SMEM)] + [pl.BlockSpec(memory_space=pltpu.VMEM)] * 2,
        out_specs=pl.BlockSpec(memory_space=pltpu.VMEM),
        scratch_shapes=[
            pltpu.VMEM((N_OWN * TILES_DEV, FIELDS * TILE, TILE), jnp.bfloat16),
            pltpu.VMEM((GROUPS, LANES), jnp.float32),
            pltpu.VMEM((GROUPS, LANES), jnp.float32),
            pltpu.VMEM((FIELDS * GROUPS * 8, LANES), jnp.float32),
        ],
        compiler_params=SMALL,
    )(header, message, column)


def following(x, lane):
    moved = pltpu.roll(x, LANES - 1, 1)
    return jnp.where(lane == LANES - 1, pltpu.roll(moved, x.shape[0] - 1, 0), moved)


def preceding(x, lane):
    moved = pltpu.roll(x, 1, 1)
    return jnp.where(lane == 0, pltpu.roll(moved, 1, 0), moved)


def flux_kernel(place_ref, before_ref, after_ref, elevation_ref, bed_ref, out_ref):
    rows = elevation_ref.shape[0]
    lane8 = iota((8, LANES), 1)
    row8 = iota((8, LANES), 0)

    def ends(which):
        before = before_ref[0, which : which + 1, :].astype(jnp.float32) * (1.0 / EDGE_SCALE)
        after = after_ref[0, which : which + 1, :].astype(jnp.float32) * (1.0 / EDGE_SCALE)
        top = jnp.where((row8 == 7) & (lane8 >= LANES - SWEEPS), before, 0.0)
        bottom = jnp.where((row8 == 0) & (lane8 < SWEEPS), after, 0.0)
        return top, bottom

    surface_top, surface_bottom = ends(5)
    bed_top, bed_bottom = ends(6)
    surface = jnp.concatenate([surface_top, elevation_ref[...], surface_bottom], axis=0)
    bed = jnp.concatenate([bed_top, bed_ref[...], bed_bottom], axis=0)
    lane = iota(surface.shape, 1)
    node = iota(surface.shape, 0) * LANES + lane
    first_wall = jnp.where(place_ref[2] == 0, 8 * LANES - 1, -1)
    last_wall = jnp.where(place_ref[2] == N_DOM - 1, (8 + rows) * LANES - 1, -1)
    open_face = jnp.where((node == first_wall) | (node == last_wall), 0.0, KAPPA)
    for sweep_step in range(SWEEPS):
        wet = jnp.maximum(surface - bed, 0.0)
        drop = surface - following(surface, lane)
        upwind = jnp.where(drop >= 0.0, wet, following(wet, lane))
        flux = open_face * upwind * drop
        surface = surface - (flux - preceding(flux, lane))
    out_ref[...] = surface[8 : 8 + rows]


def flux_sweeps(place, message, elevation, bed_level):
    whole = pl.BlockSpec(elevation.shape, lambda i, place_ref: (0, 0))
    return pl.pallas_call(
        flux_kernel,
        out_shape=jax.ShapeDtypeStruct(elevation.shape, jnp.float32),
        grid_spec=pltpu.PrefetchScalarGridSpec(
            num_scalar_prefetch=1,
            grid=(1,),
            in_specs=[
                pl.BlockSpec((1, 8, LANES), lambda i, place_ref: (place_ref[0], 1, 0)),
                pl.BlockSpec((1, 8, LANES), lambda i, place_ref: (place_ref[1], 1, 0)),
                whole,
                whole,
            ],
            out_specs=whole,
        ),
        compiler_params=SMALL,
    )(place, message, message, elevation, bed_level)


SLOTS8 = 8


def finish_kernel(need_ref, returned_ref, surface_ref, bed_ref, forcing_ref, surge_ref, stage_ref):
    rows = FIELDS * GROUPS

    def eight_slots(b, carry):
        for i in range(SLOTS8):
            s = b * SLOTS8 + i
            block = returned_ref[need_ref[0, s] % BAND // TILES_DEV].astype(jnp.float32)
            stage_ref[i * rows : (i + 1) * rows, :] = block
            here = pl.ds(pl.multiple_of(s * GROUPS, GROUPS), GROUPS)
            surface = surface_ref[here, :]
            wet = jnp.minimum(jnp.maximum(surface - bed_ref[here, :], 0.0), 1.0)
            surge_ref[here, :] = surface - 0.5 * block[rows - GROUPS :] * wet
        slots = pl.ds(pl.multiple_of(b * SLOTS8, SLOTS8), SLOTS8)
        for f in range(FIELDS):
            for g in range(GROUPS):
                piece = stage_ref[pl.ds(f * GROUPS + g, SLOTS8, stride=rows), :]
                forcing_ref[f, slots, g * LANES : (g + 1) * LANES] = piece.astype(jnp.bfloat16)
        return carry

    lax.fori_loop(0, NEED // SLOTS8, eight_slots, 0)


def finish(need_tiles, returned, surface, bed_level):
    vmem = pl.BlockSpec(memory_space=pltpu.VMEM)
    return pl.pallas_call(
        finish_kernel,
        out_shape=(
            jax.ShapeDtypeStruct((FIELDS, NEED, NPS), jnp.bfloat16),
            jax.ShapeDtypeStruct(surface.shape, jnp.float32),
        ),
        in_specs=[pl.BlockSpec(memory_space=pltpu.SMEM), vmem, vmem, vmem],
        out_specs=(vmem, vmem),
        scratch_shapes=[pltpu.VMEM((SLOTS8 * FIELDS * GROUPS, LANES), jnp.float32)],
        compiler_params=SMALL,
    )(need_tiles, returned, surface, bed_level)


def exchange(blocks, axis):
    return lax.all_to_all(blocks, axis, split_axis=0, concat_axis=0, tiled=True)


def shards(
    background, storm_track, need_tiles, node_cells, node_fracs, slot_count, elevation, bed_level
):
    own = lax.axis_index("own")
    dom = lax.axis_index("dom")
    elevation = elevation.reshape(-1, LANES)
    bed_level = bed_level.reshape(-1, LANES)
    tiles = holland((own * N_DOM + dom)[None].astype(jnp.int32), storm_track, background)
    column = lax.all_gather(tiles, "own")
    question = queries(need_tiles, slot_count, node_cells, node_fracs, elevation, bed_level)
    message = exchange(question, "dom")
    answers = interpolate(message[:, 12, 0], message, column)
    returned = exchange(answers, "dom")
    place = jnp.stack([(dom - 1) % N_DOM, (dom + 1) % N_DOM, dom]).astype(jnp.int32)
    surface = flux_sweeps(place, message, elevation, bed_level)
    forcing, surge = finish(need_tiles, returned, surface, bed_level)
    return forcing.transpose(1, 0, 2), surge.reshape(1, -1)


def solution(mesh):
    placed = (
        P(("own", "dom"), None, None),
        P(),
        P(("own", "dom"), None),
        P(("own", "dom"), None),
        P(None, ("own", "dom"), None),
        P(("own", "dom")),
        P("own", "dom"),
        P("own", "dom"),
    )
    return jax.shard_map(
        shards,
        mesh=mesh,
        in_specs=placed,
        out_specs=(P(("own", "dom"), None, None), P("own", "dom")),
        check_vma=False,
    )
```

```python
import jax
import jax.numpy as jnp
from jax import lax
from jax.experimental import pallas as pl
from jax.experimental.pallas import tpu as pltpu
from jax.sharding import PartitionSpec as P

TILE = 64
TCOLS = 32
TILES_DEV = 2
FIELDS = 6
SWEEPS = 4
KAPPA = 0.08
NEED = 32
NPS = 1024
LANES = 128
GROUPS = NPS // LANES
N_OWN = 8
N_DOM = 64
BAND = TILES_DEV * N_DOM
CORES = 2
MSG = 16
CHUNK = 256
PER_CHUNK = CHUNK // LANES
CHUNKS = NPS // CHUNK
FIELD_BITS = 10
ABSENT = (CHUNKS - 1) * FIELD_BITS << 16
LIST = 8 * FIELD_BITS
DEAD_CELL = 0xFFC0
EDGE_SCALE = 2.0**29
FX_STEP = 2.0**-16
FY_TOP = 65535.0


SMALL = pltpu.CompilerParams(vmem_limit_bytes=8 * 2**20)


def iota(shape, dim):
    return lax.broadcasted_iota(jnp.int32, shape, dim)


def storm_field(place_ref, track_ref, background_ref, out_ref, rows_ref):
    field = iota((8, LANES), 0)
    lane = iota((8, LANES), 1)
    late = field >= 3
    centre_x, centre_y, deficit, max_radius, exponent = (
        jnp.where(late, track_ref[1, i], track_ref[0, i]) for i in range(5)
    )
    kind = jnp.where(late, field - 3, field)
    strength = exponent * deficit
    left = lane < TILE

    def one_field(tile, chunk):
        tile_index = place_ref[0] * TILES_DEV + tile
        north = (tile_index // TCOLS * TILE + 2 * chunk + lane // TILE).astype(jnp.float32)
        east = (tile_index % TCOLS * TILE + lane % TILE).astype(jnp.float32)
        offset_x = east - centre_x
        offset_y = north - centre_y
        radius = jnp.sqrt(offset_x * offset_x + offset_y * offset_y + 1.0)
        ratio = jnp.exp(exponent * jnp.log(max_radius / radius))
        decay = jnp.exp(-ratio)
        speed = jnp.sqrt(strength * ratio * decay)
        wind = speed * jnp.where(kind == 0, -offset_y, offset_x) / radius
        storm = jnp.where(kind == 2, -deficit * (1.0 - decay), wind)
        piece = background_ref[:, tile, pl.ds(pl.multiple_of(chunk * LANES, LANES), LANES)]
        return piece.astype(jnp.float32) + storm[:FIELDS]

    def step(chunk, carry):
        first = one_field(0, chunk)
        second = one_field(1, chunk)
        even = jnp.where(left[:FIELDS], first, pltpu.roll(second, TILE, 1))
        odd = jnp.where(left[:FIELDS], pltpu.roll(first, TILE, 1), second)
        rows_ref[pl.ds(2 * chunk, FIELDS, stride=TILE), :] = even
        rows_ref[pl.ds(2 * chunk + 1, FIELDS, stride=TILE), :] = odd
        return carry

    lax.fori_loop(0, TILE // 2, step, 0, unroll=4)
    out_ref[...] = rows_ref[...].astype(jnp.bfloat16)


def column_code(fraction):
    scaled = fraction * 32768.0
    whole = jnp.floor(scaled)
    code = 2.0 * whole + jnp.where(scaled > whole, 1.0, 0.0)
    return jnp.minimum(code, 65535.0).astype(jnp.int32)


def row_code(fraction):
    return jnp.floor(fraction * FY_TOP + 0.5).astype(jnp.int32)


def edge_code(value):
    return jnp.floor(value * EDGE_SCALE + 0.5).astype(jnp.int32)


def prepare_kernel(
    place_ref,
    track_ref,
    need_ref,
    count_ref,
    background_ref,
    cells_ref,
    fracs_ref,
    ehead_ref,
    etail_ref,
    bhead_ref,
    btail_ref,
    tiles_ref,
    out_ref,
    rows_ref,
    stage_ref,
):
    storm_field(place_ref, track_ref, background_ref, tiles_ref, rows_ref)
    for g in range(GROUPS):
        span = slice(g * LANES, (g + 1) * LANES)
        word = cells_ref[:, span] | (column_code(fracs_ref[0, :, span]) << 16)
        stage_ref[pl.ds(g, NEED, stride=MSG), :] = word
    for g in range(GROUPS // 2):
        low = row_code(fracs_ref[1, :, g * LANES : (g + 1) * LANES])
        high = row_code(fracs_ref[1, :, NPS // 2 + g * LANES : NPS // 2 + (g + 1) * LANES])
        stage_ref[pl.ds(GROUPS + g, NEED, stride=MSG), :] = low | (high << 16)
    row = iota((8, LANES), 0)
    lane = iota((8, LANES), 1)
    position = row * LANES + lane
    surface = jnp.where(lane < SWEEPS, ehead_ref[0:1, :], etail_ref[7:8, :])
    bed = jnp.where(lane < SWEEPS, bhead_ref[0:1, :], btail_ref[7:8, :])
    plain = jnp.where(row == 5, edge_code(surface), jnp.where(row == 6, edge_code(bed), ABSENT))

    def clear(d, carry):
        out_ref[d, 8:16, :] = plain
        return carry

    lax.fori_loop(0, N_DOM, clear, 0, unroll=8)

    def place(s, carry):
        tile = need_ref[0, s]
        count = count_ref[s]
        holder = tile % BAND // TILES_DEV
        live = jnp.maximum((count + CHUNK - 1) // CHUNK, 2)
        header = (tile // BAND * TILES_DEV + tile % TILES_DEV) | ((live - 2) * FIELD_BITS << 16)
        start = pl.multiple_of(s * MSG, MSG)
        out_ref[holder, 0:8, :] = jnp.where(position < count, stage_ref[pl.ds(start, 8), :], DEAD_CELL)
        out_ref[holder, 8:16, :] = jnp.where(
            row < 4, stage_ref[pl.ds(start + 8, 8), :], jnp.where(row == 4, header, plain)
        )
        return carry

    lax.fori_loop(0, NEED, place, 0, unroll=4)


def prepare(place, storm_track, need_tiles, slot_count, background, node_cells, node_fracs, elevation, bed_level):
    last = elevation.shape[0] // 8 - 1
    head = pl.BlockSpec((8, LANES), lambda i: (0, 0))
    tail = pl.BlockSpec((8, LANES), lambda i: (last, 0))
    vmem = pl.BlockSpec(memory_space=pltpu.VMEM)
    rows = FIELDS * TILE
    return pl.pallas_call(
        prepare_kernel,
        grid=(1,),
        out_shape=(
            jax.ShapeDtypeStruct((rows, LANES), jnp.bfloat16),
            jax.ShapeDtypeStruct((N_DOM, MSG, LANES), jnp.int32),
        ),
        in_specs=[pl.BlockSpec(memory_space=pltpu.SMEM)] * 4 + [vmem] * 3 + [head, tail, head, tail],
        out_specs=(vmem, vmem),
        scratch_shapes=[
            pltpu.VMEM((rows, LANES), jnp.float32),
            pltpu.VMEM((NEED * MSG, LANES), jnp.int32),
        ],
    )(
        place,
        storm_track,
        need_tiles,
        slot_count,
        background.transpose(1, 0, 2),
        node_cells,
        node_fracs,
        elevation,
        elevation,
        bed_level,
        bed_level,
    )


SLOT_ROWS = FIELDS * GROUPS * 8


def interpolate_kernel(
    place_ref,
    header_ref,
    message_ref,
    near0,
    near1,
    near2,
    near3,
    far_ref,
    out_ref,
    tiles_ref,
    x_ref,
    y_ref,
    part_ref,
    list_ref,
):
    own = place_ref[0] // N_DOM
    for shift, ref in enumerate((near0, near1, near2, near3)):
        band = (own + N_OWN - CORES * shift) % N_OWN
        tiles_ref[2 * band] = ref[:, 0:TILE]
        tiles_ref[2 * band + 1] = ref[:, TILE : 2 * TILE]
        band = band + 1 - 2 * (band % CORES)
        tiles_ref[2 * band] = far_ref[shift, :, 0:TILE]
        tiles_ref[2 * band + 1] = far_ref[shift, :, TILE : 2 * TILE]

    packed = jnp.int32(0)
    for s in range(N_DOM):
        shift = header_ref[s] >> 16
        list_ref[shift * 8 + (lax.shift_right_logical(packed, shift) & (2**FIELD_BITS - 1))] = s
        packed = packed + (1 << shift)
    counts = [packed >> i * FIELD_BITS & (2**FIELD_BITS - 1) for i in range(CHUNKS - 1)]
    spot = iota((TILE, LANES), 0).astype(jnp.float32)

    def add_up(i, slot):
        values = []
        for f in range(FIELDS):
            at = i * SLOT_ROWS + f * 64
            pieces = [part_ref[pl.ds(at + j, GROUPS, stride=8), :] for j in range(8)]
            while len(pieces) > 1:
                pieces = [a + b for a, b in zip(pieces[::2], pieces[1::2])]
            values.append(pieces[0])
        out_ref[slot] = jnp.concatenate(values, axis=0).astype(jnp.bfloat16)

    def hat(ref, at):
        return jnp.maximum(1.0 - jnp.abs(spot - ref[at : at + 1, :]), 0.0)

    def decode(i, s):
        word = message_ref[s, 0:8, :]
        pair = message_ref[s, 8:16, :]
        cell = word & 0xFFFF
        row = (cell // TILE).astype(jnp.float32)
        low = (pair[0:4] & 0xFFFF).astype(jnp.float32)
        high = lax.shift_right_logical(pair[0:4], 16).astype(jnp.float32)
        x_ref[8 * i : 8 * i + 8, :] = (cell & (TILE - 1)).astype(jnp.float32) + lax.shift_right_logical(
            word, 16
        ).astype(jnp.float32) * FX_STEP
        y_ref[8 * i : 8 * i + 4, :] = row[0:4] + low * (1.0 / FY_TOP)
        y_ref[8 * i + 4 : 8 * i + 8, :] = row[4:8] + high * (1.0 / FY_TOP)

    def two_slots(slots, before, live):
        for i in range(2):
            add_up(i, before[i])
        for i in range(2):
            decode(i, slots[i])
        tiles = [tiles_ref[header_ref[s] & 0xFFFF] for s in slots]
        for c in range(live):
            for i in range(2):
                groups = range(c * PER_CHUNK, (c + 1) * PER_CHUNK)
                columns = jnp.concatenate([hat(x_ref, 8 * i + g).astype(jnp.bfloat16) for g in groups], axis=1)
                spread = jnp.dot(tiles[i], columns, preferred_element_type=jnp.float32)
                for j, g in enumerate(groups):
                    rows = hat(y_ref, 8 * i + g)
                    for f in range(FIELDS):
                        weighed = spread[f * TILE : (f + 1) * TILE, j * LANES : (j + 1) * LANES] * rows
                        at = i * SLOT_ROWS + (f * GROUPS + g) * 8
                        part_ref[at : at + 8, :] = jnp.sum(weighed.reshape(TILE // 8, 8, LANES), axis=0)
        dead = (CHUNKS - live) * PER_CHUNK * 8
        if dead:
            for i in range(2):
                for f in range(FIELDS):
                    at = i * SLOT_ROWS + (f + 1) * GROUPS * 8 - dead
                    part_ref[at : at + dead, :] = jnp.zeros((dead, LANES), jnp.float32)

    before = (jnp.int32(-1), jnp.int32(-1))
    for i, n in enumerate(counts):

        @pl.when(n > 0)
        def _():
            list_ref[i * LIST + n] = list_ref[i * LIST + n - 1]

        def step(p, before):
            slots = (list_ref[i * LIST + 2 * p], list_ref[i * LIST + 2 * p + 1])
            two_slots(slots, tuple(jnp.where(b < 0, s, b) for b, s in zip(before, slots)), i + 2)
            return slots

        before = lax.fori_loop(0, (n + 1) // 2, step, before)
    for i in range(2):
        add_up(i, jnp.maximum(before[i], 0))


def interpolate(place, header, message, near, far):
    return pl.pallas_call(
        interpolate_kernel,
        out_shape=jax.ShapeDtypeStruct((N_DOM, FIELDS * GROUPS, LANES), jnp.bfloat16),
        in_specs=[pl.BlockSpec(memory_space=pltpu.SMEM)] * 2 + [pl.BlockSpec(memory_space=pltpu.VMEM)] * 6,
        out_specs=pl.BlockSpec(memory_space=pltpu.VMEM),
        scratch_shapes=[
            pltpu.VMEM((N_OWN * TILES_DEV, FIELDS * TILE, TILE), jnp.bfloat16),
            pltpu.VMEM((2 * GROUPS, LANES), jnp.float32),
            pltpu.VMEM((2 * GROUPS, LANES), jnp.float32),
            pltpu.VMEM((2 * SLOT_ROWS, LANES), jnp.float32),
            pltpu.SMEM((CHUNKS * LIST,), jnp.int32),
        ],
        compiler_params=SMALL,
    )(place, header, message, *near, far)


def following(x, lane):
    moved = pltpu.roll(x, LANES - 1, 1)
    return jnp.where(lane == LANES - 1, pltpu.roll(moved, x.shape[0] - 1, 0), moved)


def preceding(x, lane):
    moved = pltpu.roll(x, 1, 1)
    return jnp.where(lane == 0, pltpu.roll(moved, 1, 0), moved)


def flux_sweeps(place_ref, before_ref, after_ref, elevation_ref, bed_ref, out_ref):
    rows = elevation_ref.shape[0]
    lane8 = iota((8, LANES), 1)
    row8 = iota((8, LANES), 0)

    def ends(which):
        before = before_ref[0, which : which + 1, :].astype(jnp.float32) * (1.0 / EDGE_SCALE)
        after = after_ref[0, which : which + 1, :].astype(jnp.float32) * (1.0 / EDGE_SCALE)
        top = jnp.where((row8 == 7) & (lane8 >= LANES - SWEEPS), before, 0.0)
        bottom = jnp.where((row8 == 0) & (lane8 < SWEEPS), after, 0.0)
        return top, bottom

    surface_top, surface_bottom = ends(5)
    bed_top, bed_bottom = ends(6)
    surface = jnp.concatenate([surface_top, elevation_ref[...], surface_bottom], axis=0)
    bed = jnp.concatenate([bed_top, bed_ref[...], bed_bottom], axis=0)
    lane = iota(surface.shape, 1)
    node = iota(surface.shape, 0) * LANES + lane
    dom = place_ref[0] % N_DOM
    first_wall = jnp.where(dom == 0, 8 * LANES - 1, -1)
    last_wall = jnp.where(dom == N_DOM - 1, (8 + rows) * LANES - 1, -1)
    open_face = jnp.where((node == first_wall) | (node == last_wall), 0.0, KAPPA)
    for _ in range(SWEEPS):
        wet = jnp.maximum(surface - bed, 0.0)
        drop = surface - following(surface, lane)
        upwind = jnp.where(drop >= 0.0, wet, following(wet, lane))
        flux = open_face * upwind * drop
        surface = surface - (flux - preceding(flux, lane))
    out_ref[...] = surface[8 : 8 + rows]


SLOTS8 = 8


def finish_kernel(
    place_ref,
    need_ref,
    returned_ref,
    before_ref,
    after_ref,
    elevation_ref,
    bed_ref,
    forcing_ref,
    surge_ref,
    surface_ref,
    stage_ref,
):
    rows = FIELDS * GROUPS
    flux_sweeps(place_ref, before_ref, after_ref, elevation_ref, bed_ref, surface_ref)

    def eight_slots(b, carry):
        for i in range(SLOTS8):
            s = b * SLOTS8 + i
            block = returned_ref[need_ref[0, s] % BAND // TILES_DEV].astype(jnp.float32)
            stage_ref[i * rows : (i + 1) * rows, :] = block
            here = pl.ds(pl.multiple_of(s * GROUPS, GROUPS), GROUPS)
            surface = surface_ref[here, :]
            wet = jnp.minimum(jnp.maximum(surface - bed_ref[here, :], 0.0), 1.0)
            surge_ref[here, :] = surface - 0.5 * block[rows - GROUPS :] * wet
        slots = pl.ds(pl.multiple_of(b * SLOTS8, SLOTS8), SLOTS8)
        for f in range(FIELDS):
            for g in range(GROUPS):
                piece = stage_ref[pl.ds(f * GROUPS + g, SLOTS8, stride=rows), :]
                forcing_ref[f, slots, g * LANES : (g + 1) * LANES] = piece.astype(jnp.bfloat16)
        return carry

    lax.fori_loop(0, NEED // SLOTS8, eight_slots, 0)


def finish(place, need_tiles, returned, message, elevation, bed_level):
    def whole(shape):
        return pl.BlockSpec(shape, lambda i, *refs: (0,) * len(shape))

    def neighbour(step):
        return pl.BlockSpec((1, 8, LANES), lambda i, place_ref, need_ref: ((place_ref[0] + step) % N_DOM, 1, 0))

    forcing = (FIELDS, NEED, NPS)
    return pl.pallas_call(
        finish_kernel,
        out_shape=(
            jax.ShapeDtypeStruct(forcing, jnp.bfloat16),
            jax.ShapeDtypeStruct(elevation.shape, jnp.float32),
        ),
        grid_spec=pltpu.PrefetchScalarGridSpec(
            num_scalar_prefetch=2,
            grid=(1,),
            in_specs=[
                whole(returned.shape),
                neighbour(N_DOM - 1),
                neighbour(1),
                whole(elevation.shape),
                whole(elevation.shape),
            ],
            out_specs=(whole(forcing), whole(elevation.shape)),
            scratch_shapes=[
                pltpu.VMEM(elevation.shape, jnp.float32),
                pltpu.VMEM((SLOTS8 * FIELDS * GROUPS, LANES), jnp.float32),
            ],
        ),
        compiler_params=SMALL,
    )(place, need_tiles, returned, message, message, elevation, bed_level)


def exchange(blocks, axis):
    return lax.all_to_all(blocks, axis, split_axis=0, concat_axis=0, tiled=True)


def shards(
    background, storm_track, need_tiles, node_cells, node_fracs, slot_count, elevation, bed_level
):
    place = (lax.axis_index("own") * N_DOM + lax.axis_index("dom"))[None].astype(jnp.int32)
    elevation = elevation.reshape(-1, LANES)
    bed_level = bed_level.reshape(-1, LANES)
    tiles, question = prepare(
        place, storm_track, need_tiles, slot_count, background, node_cells, node_fracs, elevation, bed_level
    )
    near = [tiles]
    for shift in range(CORES, N_OWN, CORES):
        near.append(lax.ppermute(tiles, "own", [(i, (i + shift) % N_OWN) for i in range(N_OWN)]))
    message = exchange(question, "dom")
    far = lax.ppermute(jnp.stack(near), "own", [(i, i ^ 1) for i in range(N_OWN)])
    answers = interpolate(place, message[:, 12, 0], message, near, far)
    returned = exchange(answers, "dom")
    forcing, surge = finish(place, need_tiles, returned, message, elevation, bed_level)
    return forcing.transpose(1, 0, 2), surge.reshape(1, -1)


def solution(mesh):
    placed = (
        P(("own", "dom"), None, None),
        P(),
        P(("own", "dom"), None),
        P(("own", "dom"), None),
        P(None, ("own", "dom"), None),
        P(("own", "dom")),
        P("own", "dom"),
        P("own", "dom"),
    )
    return jax.shard_map(
        shards,
        mesh=mesh,
        in_specs=placed,
        out_specs=(P(("own", "dom"), None, None), P("own", "dom")),
        check_vma=False,
    )
```

```python
import jax
import jax.numpy as jnp
from jax import lax
from jax.experimental import pallas as pl
from jax.experimental.pallas import tpu as pltpu
from jax.sharding import PartitionSpec as P

TILE = 64
TCOLS = 32
TILES_DEV = 2
FIELDS = 6
SWEEPS = 4
KAPPA = 0.08
NEED = 32
NPS = 1024
LANES = 128
GROUPS = NPS // LANES
N_OWN = 8
N_DOM = 64
BAND = TILES_DEV * N_DOM
CORES = 2
CHIPS = N_OWN // CORES
MSG = 16
CHUNK = 256
PER_CHUNK = CHUNK // LANES
CHUNKS = NPS // CHUNK
FIELD_BITS = 10
ABSENT = (CHUNKS - 1) * FIELD_BITS << 16
LIST = 8 * FIELD_BITS
DEAD_CELL = 0xFFC0
EDGE_SCALE = 2.0**29
FX_STEP = 2.0**-16
FY_TOP = 65535.0


SMALL = pltpu.CompilerParams(vmem_limit_bytes=8 * 2**20)


def iota(shape, dim):
    return lax.broadcasted_iota(jnp.int32, shape, dim)


def storm_field(place_ref, track_ref, background_ref, out_ref, rows_ref):
    field = iota((8, LANES), 0)
    lane = iota((8, LANES), 1)
    late = field >= 3
    centre_x, centre_y, deficit, max_radius, exponent = (
        jnp.where(late, track_ref[1, i], track_ref[0, i]) for i in range(5)
    )
    kind = jnp.where(late, field - 3, field)
    strength = exponent * deficit
    left = lane < TILE

    def one_field(tile, chunk):
        tile_index = place_ref[0] * TILES_DEV + tile
        north = (tile_index // TCOLS * TILE + 2 * chunk + lane // TILE).astype(jnp.float32)
        east = (tile_index % TCOLS * TILE + lane % TILE).astype(jnp.float32)
        offset_x = east - centre_x
        offset_y = north - centre_y
        radius = jnp.sqrt(offset_x * offset_x + offset_y * offset_y + 1.0)
        ratio = jnp.exp(exponent * jnp.log(max_radius / radius))
        decay = jnp.exp(-ratio)
        speed = jnp.sqrt(strength * ratio * decay)
        wind = speed * jnp.where(kind == 0, -offset_y, offset_x) / radius
        storm = jnp.where(kind == 2, -deficit * (1.0 - decay), wind)
        piece = background_ref[:, tile, pl.ds(pl.multiple_of(chunk * LANES, LANES), LANES)]
        return piece.astype(jnp.float32) + storm[:FIELDS]

    def step(chunk, carry):
        first = one_field(0, chunk)
        second = one_field(1, chunk)
        even = jnp.where(left[:FIELDS], first, pltpu.roll(second, TILE, 1))
        odd = jnp.where(left[:FIELDS], pltpu.roll(first, TILE, 1), second)
        rows_ref[pl.ds(2 * chunk, FIELDS, stride=TILE), :] = even
        rows_ref[pl.ds(2 * chunk + 1, FIELDS, stride=TILE), :] = odd
        return carry

    lax.fori_loop(0, TILE // 2, step, 0, unroll=8)
    out_ref[...] = rows_ref[...].astype(jnp.bfloat16)


def column_code(fraction):
    scaled = fraction * 32768.0
    whole = jnp.floor(scaled)
    code = 2.0 * whole + jnp.where(scaled > whole, 1.0, 0.0)
    return jnp.minimum(code, 65535.0).astype(jnp.int32)


def row_code(fraction):
    return jnp.floor(fraction * FY_TOP + 0.5).astype(jnp.int32)


def edge_code(value):
    return jnp.floor(value * EDGE_SCALE + 0.5).astype(jnp.int32)


def prepare_kernel(
    place_ref,
    track_ref,
    need_ref,
    count_ref,
    background_ref,
    cells_ref,
    fracs_ref,
    ehead_ref,
    etail_ref,
    bhead_ref,
    btail_ref,
    tiles_ref,
    out_ref,
    rows_ref,
    stage_ref,
):
    storm_field(place_ref, track_ref, background_ref, tiles_ref, rows_ref)
    for g in range(GROUPS):
        span = slice(g * LANES, (g + 1) * LANES)
        word = cells_ref[:, span] | (column_code(fracs_ref[0, :, span]) << 16)
        stage_ref[pl.ds(g, NEED, stride=MSG), :] = word
    for g in range(GROUPS // 2):
        low = row_code(fracs_ref[1, :, g * LANES : (g + 1) * LANES])
        high = row_code(fracs_ref[1, :, NPS // 2 + g * LANES : NPS // 2 + (g + 1) * LANES])
        stage_ref[pl.ds(GROUPS + g, NEED, stride=MSG), :] = low | (high << 16)
    row = iota((8, LANES), 0)
    lane = iota((8, LANES), 1)
    position = row * LANES + lane
    surface = jnp.where(lane < SWEEPS, ehead_ref[0:1, :], etail_ref[7:8, :])
    bed = jnp.where(lane < SWEEPS, bhead_ref[0:1, :], btail_ref[7:8, :])
    plain = jnp.where(row == 5, edge_code(surface), jnp.where(row == 6, edge_code(bed), ABSENT))

    def clear(d, carry):
        out_ref[d, 8:16, :] = plain
        return carry

    lax.fori_loop(0, N_DOM, clear, 0, unroll=8)

    def place(s, carry):
        tile = need_ref[0, s]
        count = count_ref[s]
        holder = tile % BAND // TILES_DEV
        live = jnp.maximum((count + CHUNK - 1) // CHUNK, 2)
        header = (tile // BAND * TILES_DEV + tile % TILES_DEV) | ((live - 2) * FIELD_BITS << 16)
        start = pl.multiple_of(s * MSG, MSG)
        out_ref[holder, 0:8, :] = jnp.where(position < count, stage_ref[pl.ds(start, 8), :], DEAD_CELL)
        out_ref[holder, 8:16, :] = jnp.where(
            row < 4, stage_ref[pl.ds(start + 8, 8), :], jnp.where(row == 4, header, plain)
        )
        return carry

    lax.fori_loop(0, NEED, place, 0, unroll=4)


def prepare(place, storm_track, need_tiles, slot_count, background, node_cells, node_fracs, elevation, bed_level):
    last = elevation.shape[0] // 8 - 1
    head = pl.BlockSpec((8, LANES), lambda i: (0, 0))
    tail = pl.BlockSpec((8, LANES), lambda i: (last, 0))
    vmem = pl.BlockSpec(memory_space=pltpu.VMEM)
    rows = FIELDS * TILE
    return pl.pallas_call(
        prepare_kernel,
        grid=(1,),
        out_shape=(
            jax.ShapeDtypeStruct((rows, LANES), jnp.bfloat16),
            jax.ShapeDtypeStruct((N_DOM, MSG, LANES), jnp.int32),
        ),
        in_specs=[pl.BlockSpec(memory_space=pltpu.SMEM)] * 4 + [vmem] * 3 + [head, tail, head, tail],
        out_specs=(vmem, vmem),
        scratch_shapes=[
            pltpu.VMEM((rows, LANES), jnp.float32),
            pltpu.VMEM((NEED * MSG, LANES), jnp.int32),
        ],
    )(
        place,
        storm_track,
        need_tiles,
        slot_count,
        background.transpose(1, 0, 2),
        node_cells,
        node_fracs,
        elevation,
        elevation,
        bed_level,
        bed_level,
    )


SLOT_ROWS = FIELDS * GROUPS * 8


def interpolate_kernel(
    place_ref,
    header_ref,
    message_ref,
    own_ref,
    other_ref,
    beside_ref,
    across_ref,
    far_ref,
    out_ref,
    tiles_ref,
    x_ref,
    y_ref,
    part_ref,
    list_ref,
):
    own = place_ref[0] // N_DOM
    core = own % CORES
    side = 2 * core - 1

    def keep(step, flip, ref, *index):
        z = (own // CORES + step + CHIPS) % CHIPS
        at = 2 * (z * CORES + (1 - core if flip else core))
        tiles_ref[at] = ref[(*index, slice(None), slice(0, TILE))]
        tiles_ref[at + 1] = ref[(*index, slice(None), slice(TILE, 2 * TILE))]

    keep(0, False, own_ref)
    keep(0, True, other_ref)
    keep(side, False, beside_ref, 0)
    keep(side, True, beside_ref, 1)
    keep(2, False, across_ref)
    keep(-side, True, far_ref, 0)
    keep(-side, False, far_ref, 1)
    keep(2, True, far_ref, 2)

    packed = jnp.int32(0)
    for s in range(N_DOM):
        shift = header_ref[s] >> 16
        list_ref[shift * 8 + (lax.shift_right_logical(packed, shift) & (2**FIELD_BITS - 1))] = s
        packed = packed + (1 << shift)
    counts = [packed >> i * FIELD_BITS & (2**FIELD_BITS - 1) for i in range(CHUNKS - 1)]
    spot = iota((TILE, LANES), 0).astype(jnp.float32)

    def add_up(i, slot):
        values = []
        for f in range(FIELDS):
            at = i * SLOT_ROWS + f * 64
            pieces = [part_ref[pl.ds(at + j, GROUPS, stride=8), :] for j in range(8)]
            while len(pieces) > 1:
                pieces = [a + b for a, b in zip(pieces[::2], pieces[1::2])]
            values.append(pieces[0])
        out_ref[slot] = jnp.concatenate(values, axis=0).astype(jnp.bfloat16)

    def hat(ref, at):
        return jnp.maximum(1.0 - jnp.abs(spot - ref[at : at + 1, :]), 0.0)

    def decode(i, s):
        word = message_ref[s, 0:8, :]
        pair = message_ref[s, 8:16, :]
        cell = word & 0xFFFF
        row = (cell // TILE).astype(jnp.float32)
        low = (pair[0:4] & 0xFFFF).astype(jnp.float32)
        high = lax.shift_right_logical(pair[0:4], 16).astype(jnp.float32)
        x_ref[8 * i : 8 * i + 8, :] = (cell & (TILE - 1)).astype(jnp.float32) + lax.shift_right_logical(
            word, 16
        ).astype(jnp.float32) * FX_STEP
        y_ref[8 * i : 8 * i + 4, :] = row[0:4] + low * (1.0 / FY_TOP)
        y_ref[8 * i + 4 : 8 * i + 8, :] = row[4:8] + high * (1.0 / FY_TOP)

    def two_slots(slots, before, live):
        for i in range(2):
            add_up(i, before[i])
        for i in range(2):
            decode(i, slots[i])
        tiles = [tiles_ref[header_ref[s] & 0xFFFF] for s in slots]
        for c in range(live):
            for i in range(2):
                groups = range(c * PER_CHUNK, (c + 1) * PER_CHUNK)
                columns = jnp.concatenate([hat(x_ref, 8 * i + g).astype(jnp.bfloat16) for g in groups], axis=1)
                spread = jnp.dot(tiles[i], columns, preferred_element_type=jnp.float32)
                for j, g in enumerate(groups):
                    rows = hat(y_ref, 8 * i + g)
                    for f in range(FIELDS):
                        weighed = spread[f * TILE : (f + 1) * TILE, j * LANES : (j + 1) * LANES] * rows
                        at = i * SLOT_ROWS + (f * GROUPS + g) * 8
                        part_ref[at : at + 8, :] = jnp.sum(weighed.reshape(TILE // 8, 8, LANES), axis=0)
        dead = (CHUNKS - live) * PER_CHUNK * 8
        if dead:
            for i in range(2):
                for f in range(FIELDS):
                    at = i * SLOT_ROWS + (f + 1) * GROUPS * 8 - dead
                    part_ref[at : at + dead, :] = jnp.zeros((dead, LANES), jnp.float32)

    before = (jnp.int32(-1), jnp.int32(-1))
    for i, n in enumerate(counts):

        @pl.when(n > 0)
        def _():
            list_ref[i * LIST + n] = list_ref[i * LIST + n - 1]

        def step(p, before):
            slots = (list_ref[i * LIST + 2 * p], list_ref[i * LIST + 2 * p + 1])
            two_slots(slots, tuple(jnp.where(b < 0, s, b) for b, s in zip(before, slots)), i + 2)
            return slots

        before = lax.fori_loop(0, (n + 1) // 2, step, before)
    for i in range(2):
        add_up(i, jnp.maximum(before[i], 0))


def interpolate(place, header, message, near, far):
    return pl.pallas_call(
        interpolate_kernel,
        out_shape=jax.ShapeDtypeStruct((N_DOM, FIELDS * GROUPS, LANES), jnp.bfloat16),
        in_specs=[pl.BlockSpec(memory_space=pltpu.SMEM)] * 2 + [pl.BlockSpec(memory_space=pltpu.VMEM)] * 6,
        out_specs=pl.BlockSpec(memory_space=pltpu.VMEM),
        scratch_shapes=[
            pltpu.VMEM((N_OWN * TILES_DEV, FIELDS * TILE, TILE), jnp.bfloat16),
            pltpu.VMEM((2 * GROUPS, LANES), jnp.float32),
            pltpu.VMEM((2 * GROUPS, LANES), jnp.float32),
            pltpu.VMEM((2 * SLOT_ROWS, LANES), jnp.float32),
            pltpu.SMEM((CHUNKS * LIST,), jnp.int32),
        ],
        compiler_params=SMALL,
    )(place, header, message, *near, far)


def following(x, lane):
    moved = pltpu.roll(x, LANES - 1, 1)
    return jnp.where(lane == LANES - 1, pltpu.roll(moved, x.shape[0] - 1, 0), moved)


def preceding(x, lane):
    moved = pltpu.roll(x, 1, 1)
    return jnp.where(lane == 0, pltpu.roll(moved, 1, 0), moved)


def flux_sweeps(place_ref, before_ref, after_ref, elevation_ref, bed_ref, out_ref):
    rows = elevation_ref.shape[0]
    lane8 = iota((8, LANES), 1)
    row8 = iota((8, LANES), 0)

    def ends(which):
        before = before_ref[0, which : which + 1, :].astype(jnp.float32) * (1.0 / EDGE_SCALE)
        after = after_ref[0, which : which + 1, :].astype(jnp.float32) * (1.0 / EDGE_SCALE)
        top = jnp.where((row8 == 7) & (lane8 >= LANES - SWEEPS), before, 0.0)
        bottom = jnp.where((row8 == 0) & (lane8 < SWEEPS), after, 0.0)
        return top, bottom

    surface_top, surface_bottom = ends(5)
    bed_top, bed_bottom = ends(6)
    surface = jnp.concatenate([surface_top, elevation_ref[...], surface_bottom], axis=0)
    bed = jnp.concatenate([bed_top, bed_ref[...], bed_bottom], axis=0)
    lane = iota(surface.shape, 1)
    node = iota(surface.shape, 0) * LANES + lane
    dom = place_ref[0] % N_DOM
    first_wall = jnp.where(dom == 0, 8 * LANES - 1, -1)
    last_wall = jnp.where(dom == N_DOM - 1, (8 + rows) * LANES - 1, -1)
    open_face = jnp.where((node == first_wall) | (node == last_wall), 0.0, KAPPA)
    for _ in range(SWEEPS):
        wet = jnp.maximum(surface - bed, 0.0)
        drop = surface - following(surface, lane)
        upwind = jnp.where(drop >= 0.0, wet, following(wet, lane))
        flux = open_face * upwind * drop
        surface = surface - (flux - preceding(flux, lane))
    out_ref[...] = surface[8 : 8 + rows]


SLOTS8 = 8


def finish_kernel(
    place_ref,
    need_ref,
    returned_ref,
    before_ref,
    after_ref,
    elevation_ref,
    bed_ref,
    forcing_ref,
    surge_ref,
    surface_ref,
    stage_ref,
):
    rows = FIELDS * GROUPS
    flux_sweeps(place_ref, before_ref, after_ref, elevation_ref, bed_ref, surface_ref)

    def eight_slots(b, carry):
        for i in range(SLOTS8):
            s = b * SLOTS8 + i
            block = returned_ref[need_ref[0, s] % BAND // TILES_DEV].astype(jnp.float32)
            stage_ref[i * rows : (i + 1) * rows, :] = block
            here = pl.ds(pl.multiple_of(s * GROUPS, GROUPS), GROUPS)
            surface = surface_ref[here, :]
            wet = jnp.minimum(jnp.maximum(surface - bed_ref[here, :], 0.0), 1.0)
            surge_ref[here, :] = surface - 0.5 * block[rows - GROUPS :] * wet
        slots = pl.ds(pl.multiple_of(b * SLOTS8, SLOTS8), SLOTS8)
        for f in range(FIELDS):
            for g in range(GROUPS):
                piece = stage_ref[pl.ds(f * GROUPS + g, SLOTS8, stride=rows), :]
                forcing_ref[f, slots, g * LANES : (g + 1) * LANES] = piece.astype(jnp.bfloat16)
        return carry

    lax.fori_loop(0, NEED // SLOTS8, eight_slots, 0)


def finish(place, need_tiles, returned, message, elevation, bed_level):
    def whole(shape):
        return pl.BlockSpec(shape, lambda i, *refs: (0,) * len(shape))

    def neighbour(step):
        return pl.BlockSpec((1, 8, LANES), lambda i, place_ref, need_ref: ((place_ref[0] + step) % N_DOM, 1, 0))

    forcing = (FIELDS, NEED, NPS)
    return pl.pallas_call(
        finish_kernel,
        out_shape=(
            jax.ShapeDtypeStruct(forcing, jnp.bfloat16),
            jax.ShapeDtypeStruct(elevation.shape, jnp.float32),
        ),
        grid_spec=pltpu.PrefetchScalarGridSpec(
            num_scalar_prefetch=2,
            grid=(1,),
            in_specs=[
                whole(returned.shape),
                neighbour(N_DOM - 1),
                neighbour(1),
                whole(elevation.shape),
                whole(elevation.shape),
            ],
            out_specs=(whole(forcing), whole(elevation.shape)),
            scratch_shapes=[
                pltpu.VMEM(elevation.shape, jnp.float32),
                pltpu.VMEM((SLOTS8 * FIELDS * GROUPS, LANES), jnp.float32),
            ],
        ),
        compiler_params=SMALL,
    )(place, need_tiles, returned, message, message, elevation, bed_level)


def exchange(blocks, axis):
    return lax.all_to_all(blocks, axis, split_axis=0, concat_axis=0, tiled=True)


def shards(
    background, storm_track, need_tiles, node_cells, node_fracs, slot_count, elevation, bed_level
):
    place = (lax.axis_index("own") * N_DOM + lax.axis_index("dom"))[None].astype(jnp.int32)
    elevation = elevation.reshape(-1, LANES)
    bed_level = bed_level.reshape(-1, LANES)
    tiles, question = prepare(
        place, storm_track, need_tiles, slot_count, background, node_cells, node_fracs, elevation, bed_level
    )
    other = lax.ppermute(tiles, "own", [(i, i ^ 1) for i in range(N_OWN)])
    message = exchange(question, "dom")
    turn = [(i, (i + CORES if i % CORES == 0 else i - CORES) % N_OWN) for i in range(N_OWN)]
    beside = lax.ppermute(jnp.stack([tiles, other]), "own", turn)
    across = lax.ppermute(tiles, "own", [(i, (i + 2 * CORES) % N_OWN) for i in range(N_OWN)])
    far = lax.ppermute(jnp.concatenate([beside, across[None]]), "own", [(i, i ^ 1) for i in range(N_OWN)])
    near = (tiles, other, beside, across)
    answers = interpolate(place, message[:, 12, 0], message, near, far)
    returned = exchange(answers, "dom")
    forcing, surge = finish(place, need_tiles, returned, message, elevation, bed_level)
    return forcing.transpose(1, 0, 2), surge.reshape(1, -1)


def solution(mesh):
    placed = (
        P(("own", "dom"), None, None),
        P(),
        P(("own", "dom"), None),
        P(("own", "dom"), None),
        P(None, ("own", "dom"), None),
        P(("own", "dom")),
        P("own", "dom"),
        P("own", "dom"),
    )
    return jax.shard_map(
        shards,
        mesh=mesh,
        in_specs=placed,
        out_specs=(P(("own", "dom"), None, None), P("own", "dom")),
        check_vma=False,
    )
```

```python
import jax
import jax.numpy as jnp
from jax import lax
from jax.experimental import pallas as pl
from jax.experimental.pallas import tpu as pltpu
from jax.sharding import PartitionSpec as P

TILE = 64
TCOLS = 32
TILES_DEV = 2
FIELDS = 6
SWEEPS = 4
KAPPA = 0.08
NEED = 32
NPS = 1024
LANES = 128
GROUPS = NPS // LANES
N_OWN = 8
N_DOM = 64
BAND = TILES_DEV * N_DOM
MSG = 16
CHUNK = 256
PER_CHUNK = CHUNK // LANES
CHUNKS = NPS // CHUNK
FIELD_BITS = 10
ABSENT = (CHUNKS - 1) * FIELD_BITS << 16
LIST = 8 * FIELD_BITS
DEAD_CELL = 0xFFC0
EDGE_SCALE = 2.0**29
FX_STEP = 2.0**-16
FY_TOP = 65535.0


SMALL = pltpu.CompilerParams(vmem_limit_bytes=8 * 2**20)


def iota(shape, dim):
    return lax.broadcasted_iota(jnp.int32, shape, dim)


def storm_field(place_ref, track_ref, background_ref, out_ref, rows_ref):
    field = iota((8, LANES), 0)
    lane = iota((8, LANES), 1)
    late = field >= 3
    centre_x, centre_y, deficit, max_radius, exponent = (
        jnp.where(late, track_ref[1, i], track_ref[0, i]) for i in range(5)
    )
    kind = jnp.where(late, field - 3, field)
    strength = exponent * deficit
    left = lane < TILE

    def one_field(tile, chunk):
        tile_index = place_ref[0] * TILES_DEV + tile
        north = (tile_index // TCOLS * TILE + 2 * chunk + lane // TILE).astype(jnp.float32)
        east = (tile_index % TCOLS * TILE + lane % TILE).astype(jnp.float32)
        offset_x = east - centre_x
        offset_y = north - centre_y
        radius = jnp.sqrt(offset_x * offset_x + offset_y * offset_y + 1.0)
        ratio = jnp.exp(exponent * jnp.log(max_radius / radius))
        decay = jnp.exp(-ratio)
        speed = jnp.sqrt(strength * ratio * decay)
        wind = speed * jnp.where(kind == 0, -offset_y, offset_x) / radius
        storm = jnp.where(kind == 2, -deficit * (1.0 - decay), wind)
        piece = background_ref[:, tile, pl.ds(pl.multiple_of(chunk * LANES, LANES), LANES)]
        return piece.astype(jnp.float32) + storm[:FIELDS]

    def step(chunk, carry):
        first = one_field(0, chunk)
        second = one_field(1, chunk)
        even = jnp.where(left[:FIELDS], first, pltpu.roll(second, TILE, 1))
        odd = jnp.where(left[:FIELDS], pltpu.roll(first, TILE, 1), second)
        rows_ref[pl.ds(2 * chunk, FIELDS, stride=TILE), :] = even
        rows_ref[pl.ds(2 * chunk + 1, FIELDS, stride=TILE), :] = odd
        return carry

    lax.fori_loop(0, TILE // 2, step, 0, unroll=8)
    out_ref[...] = rows_ref[...].astype(jnp.bfloat16)


def column_code(fraction):
    scaled = fraction * 32768.0
    whole = jnp.floor(scaled)
    code = 2.0 * whole + jnp.where(scaled > whole, 1.0, 0.0)
    return jnp.minimum(code, 65535.0).astype(jnp.int32)


def row_code(fraction):
    return jnp.floor(fraction * FY_TOP + 0.5).astype(jnp.int32)


def edge_code(value):
    return jnp.floor(value * EDGE_SCALE + 0.5).astype(jnp.int32)


def prepare_kernel(
    place_ref,
    track_ref,
    need_ref,
    count_ref,
    background_ref,
    cells_ref,
    fracs_ref,
    ehead_ref,
    etail_ref,
    bhead_ref,
    btail_ref,
    tiles_ref,
    out_ref,
    rows_ref,
    stage_ref,
):
    storm_field(place_ref, track_ref, background_ref, tiles_ref, rows_ref)
    for g in range(GROUPS):
        span = slice(g * LANES, (g + 1) * LANES)
        word = cells_ref[:, span] | (column_code(fracs_ref[0, :, span]) << 16)
        stage_ref[pl.ds(g, NEED, stride=MSG), :] = word
    for g in range(GROUPS // 2):
        low = row_code(fracs_ref[1, :, g * LANES : (g + 1) * LANES])
        high = row_code(fracs_ref[1, :, NPS // 2 + g * LANES : NPS // 2 + (g + 1) * LANES])
        stage_ref[pl.ds(GROUPS + g, NEED, stride=MSG), :] = low | (high << 16)
    row = iota((8, LANES), 0)
    lane = iota((8, LANES), 1)
    position = row * LANES + lane
    surface = jnp.where(lane < SWEEPS, ehead_ref[0:1, :], etail_ref[7:8, :])
    bed = jnp.where(lane < SWEEPS, bhead_ref[0:1, :], btail_ref[7:8, :])
    plain = jnp.where(row == 5, edge_code(surface), jnp.where(row == 6, edge_code(bed), ABSENT))

    def clear(d, carry):
        out_ref[d, 8:16, :] = plain
        return carry

    lax.fori_loop(0, N_DOM, clear, 0, unroll=8)

    def place(s, carry):
        tile = need_ref[0, s]
        count = count_ref[s]
        holder = tile % BAND // TILES_DEV
        live = jnp.maximum((count + CHUNK - 1) // CHUNK, 2)
        header = (tile // BAND * TILES_DEV + tile % TILES_DEV) | ((live - 2) * FIELD_BITS << 16)
        start = pl.multiple_of(s * MSG, MSG)
        out_ref[holder, 0:8, :] = jnp.where(position < count, stage_ref[pl.ds(start, 8), :], DEAD_CELL)
        out_ref[holder, 8:16, :] = jnp.where(
            row < 4, stage_ref[pl.ds(start + 8, 8), :], jnp.where(row == 4, header, plain)
        )
        return carry

    lax.fori_loop(0, NEED, place, 0, unroll=4)


def prepare(place, storm_track, need_tiles, slot_count, background, node_cells, node_fracs, elevation, bed_level):
    last = elevation.shape[0] // 8 - 1
    head = pl.BlockSpec((8, LANES), lambda i: (0, 0))
    tail = pl.BlockSpec((8, LANES), lambda i: (last, 0))
    vmem = pl.BlockSpec(memory_space=pltpu.VMEM)
    rows = FIELDS * TILE
    return pl.pallas_call(
        prepare_kernel,
        grid=(1,),
        out_shape=(
            jax.ShapeDtypeStruct((rows, LANES), jnp.bfloat16),
            jax.ShapeDtypeStruct((N_DOM, MSG, LANES), jnp.int32),
        ),
        in_specs=[pl.BlockSpec(memory_space=pltpu.SMEM)] * 4 + [vmem] * 3 + [head, tail, head, tail],
        out_specs=(vmem, vmem),
        scratch_shapes=[
            pltpu.VMEM((rows, LANES), jnp.float32),
            pltpu.VMEM((NEED * MSG, LANES), jnp.int32),
        ],
    )(
        place,
        storm_track,
        need_tiles,
        slot_count,
        background.transpose(1, 0, 2),
        node_cells,
        node_fracs,
        elevation,
        elevation,
        bed_level,
        bed_level,
    )


SLOT_ROWS = FIELDS * GROUPS * 8


def interpolate_kernel(
    header_ref,
    message_ref,
    column_ref,
    out_ref,
    tiles_ref,
    x_ref,
    y_ref,
    part_ref,
    list_ref,
):
    for k in range(N_OWN):
        tiles_ref[2 * k] = column_ref[k, :, 0:TILE]
        tiles_ref[2 * k + 1] = column_ref[k, :, TILE : 2 * TILE]

    packed = jnp.int32(0)
    for s in range(N_DOM):
        shift = header_ref[s] >> 16
        list_ref[shift * 8 + (lax.shift_right_logical(packed, shift) & (2**FIELD_BITS - 1))] = s
        packed = packed + (1 << shift)
    counts = [packed >> i * FIELD_BITS & (2**FIELD_BITS - 1) for i in range(CHUNKS - 1)]
    spot = iota((TILE, LANES), 0).astype(jnp.float32)

    def add_up(i, slot):
        values = []
        for f in range(FIELDS):
            at = i * SLOT_ROWS + f * 64
            pieces = [part_ref[pl.ds(at + j, GROUPS, stride=8), :] for j in range(8)]
            while len(pieces) > 1:
                pieces = [a + b for a, b in zip(pieces[::2], pieces[1::2])]
            values.append(pieces[0])
        out_ref[slot] = jnp.concatenate(values, axis=0).astype(jnp.bfloat16)

    def hat(ref, at):
        return jnp.maximum(1.0 - jnp.abs(spot - ref[at : at + 1, :]), 0.0)

    def decode(i, s):
        word = message_ref[s, 0:8, :]
        pair = message_ref[s, 8:16, :]
        cell = word & 0xFFFF
        row = (cell // TILE).astype(jnp.float32)
        low = (pair[0:4] & 0xFFFF).astype(jnp.float32)
        high = lax.shift_right_logical(pair[0:4], 16).astype(jnp.float32)
        x_ref[8 * i : 8 * i + 8, :] = (cell & (TILE - 1)).astype(jnp.float32) + lax.shift_right_logical(
            word, 16
        ).astype(jnp.float32) * FX_STEP
        y_ref[8 * i : 8 * i + 4, :] = row[0:4] + low * (1.0 / FY_TOP)
        y_ref[8 * i + 4 : 8 * i + 8, :] = row[4:8] + high * (1.0 / FY_TOP)

    def two_slots(slots, before, live):
        for i in range(2):
            add_up(i, before[i])
        for i in range(2):
            decode(i, slots[i])
        tiles = [tiles_ref[header_ref[s] & 0xFFFF] for s in slots]
        for c in range(live):
            for i in range(2):
                groups = range(c * PER_CHUNK, (c + 1) * PER_CHUNK)
                columns = jnp.concatenate([hat(x_ref, 8 * i + g).astype(jnp.bfloat16) for g in groups], axis=1)
                spread = jnp.dot(tiles[i], columns, preferred_element_type=jnp.float32)
                for j, g in enumerate(groups):
                    rows = hat(y_ref, 8 * i + g)
                    for f in range(FIELDS):
                        weighed = spread[f * TILE : (f + 1) * TILE, j * LANES : (j + 1) * LANES] * rows
                        at = i * SLOT_ROWS + (f * GROUPS + g) * 8
                        part_ref[at : at + 8, :] = jnp.sum(weighed.reshape(TILE // 8, 8, LANES), axis=0)
        dead = (CHUNKS - live) * PER_CHUNK * 8
        if dead:
            for i in range(2):
                for f in range(FIELDS):
                    at = i * SLOT_ROWS + (f + 1) * GROUPS * 8 - dead
                    part_ref[at : at + dead, :] = jnp.zeros((dead, LANES), jnp.float32)

    before = (jnp.int32(-1), jnp.int32(-1))
    for i, n in enumerate(counts):

        @pl.when(n > 0)
        def _():
            list_ref[i * LIST + n] = list_ref[i * LIST + n - 1]

        def step(p, before):
            slots = (list_ref[i * LIST + 2 * p], list_ref[i * LIST + 2 * p + 1])
            two_slots(slots, tuple(jnp.where(b < 0, s, b) for b, s in zip(before, slots)), i + 2)
            return slots

        before = lax.fori_loop(0, (n + 1) // 2, step, before)
    for i in range(2):
        add_up(i, jnp.maximum(before[i], 0))


def interpolate(header, message, column):
    return pl.pallas_call(
        interpolate_kernel,
        out_shape=jax.ShapeDtypeStruct((N_DOM, FIELDS * GROUPS, LANES), jnp.bfloat16),
        in_specs=[pl.BlockSpec(memory_space=pltpu.SMEM)] + [pl.BlockSpec(memory_space=pltpu.VMEM)] * 2,
        out_specs=pl.BlockSpec(memory_space=pltpu.VMEM),
        scratch_shapes=[
            pltpu.VMEM((N_OWN * TILES_DEV, FIELDS * TILE, TILE), jnp.bfloat16),
            pltpu.VMEM((2 * GROUPS, LANES), jnp.float32),
            pltpu.VMEM((2 * GROUPS, LANES), jnp.float32),
            pltpu.VMEM((2 * SLOT_ROWS, LANES), jnp.float32),
            pltpu.SMEM((CHUNKS * LIST,), jnp.int32),
        ],
        compiler_params=SMALL,
    )(header, message, column)


def following(x, lane):
    moved = pltpu.roll(x, LANES - 1, 1)
    return jnp.where(lane == LANES - 1, pltpu.roll(moved, x.shape[0] - 1, 0), moved)


def preceding(x, lane):
    moved = pltpu.roll(x, 1, 1)
    return jnp.where(lane == 0, pltpu.roll(moved, 1, 0), moved)


def flux_sweeps(place_ref, before_ref, after_ref, elevation_ref, bed_ref, out_ref):
    rows = elevation_ref.shape[0]
    lane8 = iota((8, LANES), 1)
    row8 = iota((8, LANES), 0)

    def ends(which):
        before = before_ref[0, which : which + 1, :].astype(jnp.float32) * (1.0 / EDGE_SCALE)
        after = after_ref[0, which : which + 1, :].astype(jnp.float32) * (1.0 / EDGE_SCALE)
        top = jnp.where((row8 == 7) & (lane8 >= LANES - SWEEPS), before, 0.0)
        bottom = jnp.where((row8 == 0) & (lane8 < SWEEPS), after, 0.0)
        return top, bottom

    surface_top, surface_bottom = ends(5)
    bed_top, bed_bottom = ends(6)
    surface = jnp.concatenate([surface_top, elevation_ref[...], surface_bottom], axis=0)
    bed = jnp.concatenate([bed_top, bed_ref[...], bed_bottom], axis=0)
    lane = iota(surface.shape, 1)
    node = iota(surface.shape, 0) * LANES + lane
    dom = place_ref[0] % N_DOM
    first_wall = jnp.where(dom == 0, 8 * LANES - 1, -1)
    last_wall = jnp.where(dom == N_DOM - 1, (8 + rows) * LANES - 1, -1)
    open_face = jnp.where((node == first_wall) | (node == last_wall), 0.0, KAPPA)
    for _ in range(SWEEPS):
        wet = jnp.maximum(surface - bed, 0.0)
        drop = surface - following(surface, lane)
        upwind = jnp.where(drop >= 0.0, wet, following(wet, lane))
        flux = open_face * upwind * drop
        surface = surface - (flux - preceding(flux, lane))
    out_ref[...] = surface[8 : 8 + rows]


SLOTS8 = 8


def finish_kernel(
    place_ref,
    need_ref,
    returned_ref,
    before_ref,
    after_ref,
    elevation_ref,
    bed_ref,
    forcing_ref,
    surge_ref,
    surface_ref,
    stage_ref,
):
    rows = FIELDS * GROUPS
    flux_sweeps(place_ref, before_ref, after_ref, elevation_ref, bed_ref, surface_ref)

    def eight_slots(b, carry):
        for i in range(SLOTS8):
            s = b * SLOTS8 + i
            block = returned_ref[need_ref[0, s] % BAND // TILES_DEV].astype(jnp.float32)
            stage_ref[i * rows : (i + 1) * rows, :] = block
            here = pl.ds(pl.multiple_of(s * GROUPS, GROUPS), GROUPS)
            surface = surface_ref[here, :]
            wet = jnp.minimum(jnp.maximum(surface - bed_ref[here, :], 0.0), 1.0)
            surge_ref[here, :] = surface - 0.5 * block[rows - GROUPS :] * wet
        slots = pl.ds(pl.multiple_of(b * SLOTS8, SLOTS8), SLOTS8)
        for f in range(FIELDS):
            for g in range(GROUPS):
                piece = stage_ref[pl.ds(f * GROUPS + g, SLOTS8, stride=rows), :]
                forcing_ref[f, slots, g * LANES : (g + 1) * LANES] = piece.astype(jnp.bfloat16)
        return carry

    lax.fori_loop(0, NEED // SLOTS8, eight_slots, 0)


def finish(place, need_tiles, returned, message, elevation, bed_level):
    def whole(shape):
        return pl.BlockSpec(shape, lambda i, *refs: (0,) * len(shape))

    def neighbour(step):
        return pl.BlockSpec((1, 8, LANES), lambda i, place_ref, need_ref: ((place_ref[0] + step) % N_DOM, 1, 0))

    forcing = (FIELDS, NEED, NPS)
    return pl.pallas_call(
        finish_kernel,
        out_shape=(
            jax.ShapeDtypeStruct(forcing, jnp.bfloat16),
            jax.ShapeDtypeStruct(elevation.shape, jnp.float32),
        ),
        grid_spec=pltpu.PrefetchScalarGridSpec(
            num_scalar_prefetch=2,
            grid=(1,),
            in_specs=[
                whole(returned.shape),
                neighbour(N_DOM - 1),
                neighbour(1),
                whole(elevation.shape),
                whole(elevation.shape),
            ],
            out_specs=(whole(forcing), whole(elevation.shape)),
            scratch_shapes=[
                pltpu.VMEM(elevation.shape, jnp.float32),
                pltpu.VMEM((SLOTS8 * FIELDS * GROUPS, LANES), jnp.float32),
            ],
        ),
        compiler_params=SMALL,
    )(place, need_tiles, returned, message, message, elevation, bed_level)


def exchange(blocks, axis):
    return lax.all_to_all(blocks, axis, split_axis=0, concat_axis=0, tiled=True)


def shards(
    background, storm_track, need_tiles, node_cells, node_fracs, slot_count, elevation, bed_level
):
    place = (lax.axis_index("own") * N_DOM + lax.axis_index("dom"))[None].astype(jnp.int32)
    elevation = elevation.reshape(-1, LANES)
    bed_level = bed_level.reshape(-1, LANES)
    tiles, question = prepare(
        place, storm_track, need_tiles, slot_count, background, node_cells, node_fracs, elevation, bed_level
    )
    message = exchange(question, "dom")
    column = lax.all_gather(tiles, "own")
    answers = interpolate(message[:, 12, 0], message, column)
    returned = exchange(answers, "dom")
    forcing, surge = finish(place, need_tiles, returned, message, elevation, bed_level)
    return forcing.transpose(1, 0, 2), surge.reshape(1, -1)


def solution(mesh):
    placed = (
        P(("own", "dom"), None, None),
        P(),
        P(("own", "dom"), None),
        P(("own", "dom"), None),
        P(None, ("own", "dom"), None),
        P(("own", "dom")),
        P("own", "dom"),
        P("own", "dom"),
    )
    return jax.shard_map(
        shards,
        mesh=mesh,
        in_specs=placed,
        out_specs=(P(("own", "dom"), None, None), P("own", "dom")),
        check_vma=False,
    )
```

```python
import jax
import jax.numpy as jnp
from jax import lax
from jax.experimental import pallas as pl
from jax.experimental.pallas import tpu as pltpu
from jax.sharding import PartitionSpec as P

TILE = 64
TCOLS = 32
TILES_DEV = 2
FIELDS = 6
SWEEPS = 4
KAPPA = 0.08
NEED = 32
NPS = 1024
LANES = 128
GROUPS = NPS // LANES
N_OWN = 8
N_DOM = 64
BAND = TILES_DEV * N_DOM
CORES = 2
MSG = 16
CHUNK = 256
PER_CHUNK = CHUNK // LANES
CHUNKS = NPS // CHUNK
FIELD_BITS = 10
ABSENT = (CHUNKS - 1) * FIELD_BITS << 16
LIST = 8 * FIELD_BITS
DEAD_CELL = 0xFFC0
EDGE_SCALE = 2.0**29
FX_STEP = 2.0**-16
FY_TOP = 65535.0


SMALL = pltpu.CompilerParams(vmem_limit_bytes=8 * 2**20)


def iota(shape, dim):
    return lax.broadcasted_iota(jnp.int32, shape, dim)


def storm_field(place_ref, track_ref, background_ref, out_ref, rows_ref):
    field = iota((8, LANES), 0)
    lane = iota((8, LANES), 1)
    late = field >= 3
    centre_x, centre_y, deficit, max_radius, exponent = (
        jnp.where(late, track_ref[1, i], track_ref[0, i]) for i in range(5)
    )
    kind = jnp.where(late, field - 3, field)
    strength = exponent * deficit
    left = lane < TILE

    def one_field(tile, chunk):
        tile_index = place_ref[0] * TILES_DEV + tile
        north = (tile_index // TCOLS * TILE + 2 * chunk + lane // TILE).astype(jnp.float32)
        east = (tile_index % TCOLS * TILE + lane % TILE).astype(jnp.float32)
        offset_x = east - centre_x
        offset_y = north - centre_y
        radius = jnp.sqrt(offset_x * offset_x + offset_y * offset_y + 1.0)
        ratio = jnp.exp(exponent * jnp.log(max_radius / radius))
        decay = jnp.exp(-ratio)
        speed = jnp.sqrt(strength * ratio * decay)
        wind = speed * jnp.where(kind == 0, -offset_y, offset_x) / radius
        storm = jnp.where(kind == 2, -deficit * (1.0 - decay), wind)
        piece = background_ref[:, tile, pl.ds(pl.multiple_of(chunk * LANES, LANES), LANES)]
        return piece.astype(jnp.float32) + storm[:FIELDS]

    def step(chunk, carry):
        first = one_field(0, chunk)
        second = one_field(1, chunk)
        even = jnp.where(left[:FIELDS], first, pltpu.roll(second, TILE, 1))
        odd = jnp.where(left[:FIELDS], pltpu.roll(first, TILE, 1), second)
        rows_ref[pl.ds(2 * chunk, FIELDS, stride=TILE), :] = even
        rows_ref[pl.ds(2 * chunk + 1, FIELDS, stride=TILE), :] = odd
        return carry

    lax.fori_loop(0, TILE // 2, step, 0, unroll=8)
    out_ref[...] = rows_ref[...].astype(jnp.bfloat16)


def column_code(fraction):
    scaled = fraction * 32768.0
    whole = jnp.floor(scaled)
    code = 2.0 * whole + jnp.where(scaled > whole, 1.0, 0.0)
    return jnp.minimum(code, 65535.0).astype(jnp.int32)


def row_code(fraction):
    return jnp.floor(fraction * FY_TOP + 0.5).astype(jnp.int32)


def edge_code(value):
    return jnp.floor(value * EDGE_SCALE + 0.5).astype(jnp.int32)


def prepare_kernel(
    place_ref,
    track_ref,
    need_ref,
    count_ref,
    background_ref,
    cells_ref,
    fracs_ref,
    ehead_ref,
    etail_ref,
    bhead_ref,
    btail_ref,
    tiles_ref,
    out_ref,
    rows_ref,
    stage_ref,
):
    storm_field(place_ref, track_ref, background_ref, tiles_ref, rows_ref)
    for g in range(GROUPS):
        span = slice(g * LANES, (g + 1) * LANES)
        word = cells_ref[:, span] | (column_code(fracs_ref[0, :, span]) << 16)
        stage_ref[pl.ds(g, NEED, stride=MSG), :] = word
    for g in range(GROUPS // 2):
        low = row_code(fracs_ref[1, :, g * LANES : (g + 1) * LANES])
        high = row_code(fracs_ref[1, :, NPS // 2 + g * LANES : NPS // 2 + (g + 1) * LANES])
        stage_ref[pl.ds(GROUPS + g, NEED, stride=MSG), :] = low | (high << 16)
    row = iota((8, LANES), 0)
    lane = iota((8, LANES), 1)
    position = row * LANES + lane
    surface = jnp.where(lane < SWEEPS, ehead_ref[0:1, :], etail_ref[7:8, :])
    bed = jnp.where(lane < SWEEPS, bhead_ref[0:1, :], btail_ref[7:8, :])
    plain = jnp.where(row == 5, edge_code(surface), jnp.where(row == 6, edge_code(bed), ABSENT))

    def clear(d, carry):
        out_ref[d, 8:16, :] = plain
        return carry

    lax.fori_loop(0, N_DOM, clear, 0, unroll=8)

    def place(s, carry):
        tile = need_ref[0, s]
        count = count_ref[s]
        holder = tile % BAND // TILES_DEV
        live = jnp.maximum((count + CHUNK - 1) // CHUNK, 2)
        header = (tile // BAND * TILES_DEV + tile % TILES_DEV) | ((live - 2) * FIELD_BITS << 16)
        start = pl.multiple_of(s * MSG, MSG)
        out_ref[holder, 0:8, :] = jnp.where(position < count, stage_ref[pl.ds(start, 8), :], DEAD_CELL)
        out_ref[holder, 8:16, :] = jnp.where(
            row < 4, stage_ref[pl.ds(start + 8, 8), :], jnp.where(row == 4, header, plain)
        )
        return carry

    lax.fori_loop(0, NEED, place, 0, unroll=4)


def prepare(place, storm_track, need_tiles, slot_count, background, node_cells, node_fracs, elevation, bed_level):
    last = elevation.shape[0] // 8 - 1
    head = pl.BlockSpec((8, LANES), lambda i: (0, 0))
    tail = pl.BlockSpec((8, LANES), lambda i: (last, 0))
    vmem = pl.BlockSpec(memory_space=pltpu.VMEM)
    rows = FIELDS * TILE
    return pl.pallas_call(
        prepare_kernel,
        grid=(1,),
        out_shape=(
            jax.ShapeDtypeStruct((rows, LANES), jnp.bfloat16),
            jax.ShapeDtypeStruct((N_DOM, MSG, LANES), jnp.int32),
        ),
        in_specs=[pl.BlockSpec(memory_space=pltpu.SMEM)] * 4 + [vmem] * 3 + [head, tail, head, tail],
        out_specs=(vmem, vmem),
        scratch_shapes=[
            pltpu.VMEM((rows, LANES), jnp.float32),
            pltpu.VMEM((NEED * MSG, LANES), jnp.int32),
        ],
    )(
        place,
        storm_track,
        need_tiles,
        slot_count,
        background.transpose(1, 0, 2),
        node_cells,
        node_fracs,
        elevation,
        elevation,
        bed_level,
        bed_level,
    )


SLOT_ROWS = FIELDS * GROUPS * 8
HALF = FIELDS // 2


def interpolate_kernel(
    place_ref,
    header_ref,
    message_ref,
    near0,
    near1,
    near2,
    near3,
    far_ref,
    out_ref,
    tiles_ref,
    x_ref,
    y_ref,
    part_ref,
    list_ref,
):
    own = place_ref[0] // N_DOM

    def keep(band, pair):
        tiles_ref[2 * band] = pair
        tiles_ref[2 * band + 1] = pltpu.roll(pair, TILE, 1)

    for shift, ref in enumerate((near0, near1, near2, near3)):
        band = (own + N_OWN - CORES * shift) % N_OWN
        keep(band, ref[...])
        keep(band + 1 - 2 * (band % CORES), far_ref[shift])

    packed = jnp.int32(0)
    for s in range(N_DOM):
        shift = header_ref[s] >> 16
        list_ref[shift * 8 + (lax.shift_right_logical(packed, shift) & (2**FIELD_BITS - 1))] = s
        packed = packed + (1 << shift)
    counts = [packed >> i * FIELD_BITS & (2**FIELD_BITS - 1) for i in range(CHUNKS - 1)]
    spot = iota((TILE, LANES), 0).astype(jnp.float32)

    def add_up(i, slot):
        values = []
        for f in range(FIELDS):
            at = i * SLOT_ROWS + f * 64
            pieces = [part_ref[pl.ds(at + j, GROUPS, stride=8), :] for j in range(8)]
            while len(pieces) > 1:
                pieces = [a + b for a, b in zip(pieces[::2], pieces[1::2])]
            values.append(pieces[0])
        out_ref[slot] = jnp.concatenate(values, axis=0).astype(jnp.bfloat16)

    def hat(ref, at):
        return jnp.maximum(1.0 - jnp.abs(spot - ref[at : at + 1, :]), 0.0)

    def decode(i, s):
        word = message_ref[s, 0:8, :]
        pair = message_ref[s, 8:16, :]
        cell = word & 0xFFFF
        row = (cell // TILE).astype(jnp.float32)
        low = (pair[0:4] & 0xFFFF).astype(jnp.float32)
        high = lax.shift_right_logical(pair[0:4], 16).astype(jnp.float32)
        x_ref[8 * i : 8 * i + 8, :] = (cell & (TILE - 1)).astype(jnp.float32) + lax.shift_right_logical(
            word, 16
        ).astype(jnp.float32) * FX_STEP
        y_ref[8 * i : 8 * i + 4, :] = row[0:4] + low * (1.0 / FY_TOP)
        y_ref[8 * i + 4 : 8 * i + 8, :] = row[4:8] + high * (1.0 / FY_TOP)

    def two_slots(slots, before, live):
        for i in range(2):
            add_up(i, before[i])
        for i in range(2):
            decode(i, slots[i])
        tiles = [tiles_ref[header_ref[s] & 0xFFFF, :, 0:TILE] for s in slots]
        for c in range(live):
            for i in range(2):
                groups = range(c * PER_CHUNK, (c + 1) * PER_CHUNK)
                columns = jnp.concatenate([hat(x_ref, 8 * i + g).astype(jnp.bfloat16) for g in groups], axis=1)
                rows = jnp.concatenate([hat(y_ref, 8 * i + g) for g in groups], axis=1)
                for f in range(FIELDS):
                    if f % HALF == 0:
                        part = tiles[i][f * TILE : (f + HALF) * TILE]
                        spread = jnp.dot(part, columns, preferred_element_type=jnp.float32)
                    weighed = spread[f % HALF * TILE : (f % HALF + 1) * TILE] * rows
                    total = jnp.sum(weighed.reshape(TILE // 8, 8, CHUNK), axis=0)
                    for j, g in enumerate(groups):
                        at = i * SLOT_ROWS + (f * GROUPS + g) * 8
                        part_ref[at : at + 8, :] = total[:, j * LANES : (j + 1) * LANES]
        dead = (CHUNKS - live) * PER_CHUNK * 8
        if dead:
            for i in range(2):
                for f in range(FIELDS):
                    at = i * SLOT_ROWS + (f + 1) * GROUPS * 8 - dead
                    part_ref[at : at + dead, :] = jnp.zeros((dead, LANES), jnp.float32)

    before = (jnp.int32(-1), jnp.int32(-1))
    for i, n in enumerate(counts):

        @pl.when(n > 0)
        def _():
            list_ref[i * LIST + n] = list_ref[i * LIST + n - 1]

        def step(p, before):
            slots = (list_ref[i * LIST + 2 * p], list_ref[i * LIST + 2 * p + 1])
            two_slots(slots, tuple(jnp.where(b < 0, s, b) for b, s in zip(before, slots)), i + 2)
            return slots

        before = lax.fori_loop(0, (n + 1) // 2, step, before)
    for i in range(2):
        add_up(i, jnp.maximum(before[i], 0))


def interpolate(place, header, message, near, far):
    return pl.pallas_call(
        interpolate_kernel,
        out_shape=jax.ShapeDtypeStruct((N_DOM, FIELDS * GROUPS, LANES), jnp.bfloat16),
        in_specs=[pl.BlockSpec(memory_space=pltpu.SMEM)] * 2 + [pl.BlockSpec(memory_space=pltpu.VMEM)] * 6,
        out_specs=pl.BlockSpec(memory_space=pltpu.VMEM),
        scratch_shapes=[
            pltpu.VMEM((N_OWN * TILES_DEV, FIELDS * TILE, LANES), jnp.bfloat16),
            pltpu.VMEM((2 * GROUPS, LANES), jnp.float32),
            pltpu.VMEM((2 * GROUPS, LANES), jnp.float32),
            pltpu.VMEM((2 * SLOT_ROWS, LANES), jnp.float32),
            pltpu.SMEM((CHUNKS * LIST,), jnp.int32),
        ],
        compiler_params=SMALL,
    )(place, header, message, *near, far)


def following(x, lane):
    moved = pltpu.roll(x, LANES - 1, 1)
    return jnp.where(lane == LANES - 1, pltpu.roll(moved, x.shape[0] - 1, 0), moved)


def preceding(x, lane):
    moved = pltpu.roll(x, 1, 1)
    return jnp.where(lane == 0, pltpu.roll(moved, 1, 0), moved)


def flux_sweeps(place_ref, before_ref, after_ref, elevation_ref, bed_ref, out_ref):
    rows = elevation_ref.shape[0]
    lane8 = iota((8, LANES), 1)
    row8 = iota((8, LANES), 0)

    def ends(which):
        before = before_ref[0, which : which + 1, :].astype(jnp.float32) * (1.0 / EDGE_SCALE)
        after = after_ref[0, which : which + 1, :].astype(jnp.float32) * (1.0 / EDGE_SCALE)
        top = jnp.where((row8 == 7) & (lane8 >= LANES - SWEEPS), before, 0.0)
        bottom = jnp.where((row8 == 0) & (lane8 < SWEEPS), after, 0.0)
        return top, bottom

    surface_top, surface_bottom = ends(5)
    bed_top, bed_bottom = ends(6)
    surface = jnp.concatenate([surface_top, elevation_ref[...], surface_bottom], axis=0)
    bed = jnp.concatenate([bed_top, bed_ref[...], bed_bottom], axis=0)
    lane = iota(surface.shape, 1)
    node = iota(surface.shape, 0) * LANES + lane
    dom = place_ref[0] % N_DOM
    first_wall = jnp.where(dom == 0, 8 * LANES - 1, -1)
    last_wall = jnp.where(dom == N_DOM - 1, (8 + rows) * LANES - 1, -1)
    open_face = jnp.where((node == first_wall) | (node == last_wall), 0.0, KAPPA)
    for _ in range(SWEEPS):
        wet = jnp.maximum(surface - bed, 0.0)
        drop = surface - following(surface, lane)
        upwind = jnp.where(drop >= 0.0, wet, following(wet, lane))
        flux = open_face * upwind * drop
        surface = surface - (flux - preceding(flux, lane))
    out_ref[...] = surface[8 : 8 + rows]


SLOTS8 = 8


def finish_kernel(
    place_ref,
    need_ref,
    returned_ref,
    before_ref,
    after_ref,
    elevation_ref,
    bed_ref,
    forcing_ref,
    surge_ref,
    surface_ref,
    stage_ref,
):
    rows = FIELDS * GROUPS
    flux_sweeps(place_ref, before_ref, after_ref, elevation_ref, bed_ref, surface_ref)

    def eight_slots(b, carry):
        for i in range(SLOTS8):
            s = b * SLOTS8 + i
            block = returned_ref[need_ref[0, s] % BAND // TILES_DEV].astype(jnp.float32)
            stage_ref[i * rows : (i + 1) * rows, :] = block
            here = pl.ds(pl.multiple_of(s * GROUPS, GROUPS), GROUPS)
            surface = surface_ref[here, :]
            wet = jnp.minimum(jnp.maximum(surface - bed_ref[here, :], 0.0), 1.0)
            surge_ref[here, :] = surface - 0.5 * block[rows - GROUPS :] * wet
        slots = pl.ds(pl.multiple_of(b * SLOTS8, SLOTS8), SLOTS8)
        for f in range(FIELDS):
            for g in range(GROUPS):
                piece = stage_ref[pl.ds(f * GROUPS + g, SLOTS8, stride=rows), :]
                forcing_ref[f, slots, g * LANES : (g + 1) * LANES] = piece.astype(jnp.bfloat16)
        return carry

    lax.fori_loop(0, NEED // SLOTS8, eight_slots, 0)


def finish(place, need_tiles, returned, message, elevation, bed_level):
    def whole(shape):
        return pl.BlockSpec(shape, lambda i, *refs: (0,) * len(shape))

    def neighbour(step):
        return pl.BlockSpec((1, 8, LANES), lambda i, place_ref, need_ref: ((place_ref[0] + step) % N_DOM, 1, 0))

    forcing = (FIELDS, NEED, NPS)
    return pl.pallas_call(
        finish_kernel,
        out_shape=(
            jax.ShapeDtypeStruct(forcing, jnp.bfloat16),
            jax.ShapeDtypeStruct(elevation.shape, jnp.float32),
        ),
        grid_spec=pltpu.PrefetchScalarGridSpec(
            num_scalar_prefetch=2,
            grid=(1,),
            in_specs=[
                whole(returned.shape),
                neighbour(N_DOM - 1),
                neighbour(1),
                whole(elevation.shape),
                whole(elevation.shape),
            ],
            out_specs=(whole(forcing), whole(elevation.shape)),
            scratch_shapes=[
                pltpu.VMEM(elevation.shape, jnp.float32),
                pltpu.VMEM((SLOTS8 * FIELDS * GROUPS, LANES), jnp.float32),
            ],
        ),
        compiler_params=SMALL,
    )(place, need_tiles, returned, message, message, elevation, bed_level)


def exchange(blocks, axis):
    return lax.all_to_all(blocks, axis, split_axis=0, concat_axis=0, tiled=True)


def shards(
    background, storm_track, need_tiles, node_cells, node_fracs, slot_count, elevation, bed_level
):
    place = (lax.axis_index("own") * N_DOM + lax.axis_index("dom"))[None].astype(jnp.int32)
    elevation = elevation.reshape(-1, LANES)
    bed_level = bed_level.reshape(-1, LANES)
    tiles, question = prepare(
        place, storm_track, need_tiles, slot_count, background, node_cells, node_fracs, elevation, bed_level
    )
    near = [tiles]
    for shift in range(CORES, N_OWN, CORES):
        near.append(lax.ppermute(tiles, "own", [(i, (i + shift) % N_OWN) for i in range(N_OWN)]))
    message = exchange(question, "dom")
    far = lax.ppermute(jnp.stack(near), "own", [(i, i ^ 1) for i in range(N_OWN)])
    answers = interpolate(place, message[:, 12, 0], message, near, far)
    returned = exchange(answers, "dom")
    forcing, surge = finish(place, need_tiles, returned, message, elevation, bed_level)
    return forcing.transpose(1, 0, 2), surge.reshape(1, -1)


def solution(mesh):
    placed = (
        P(("own", "dom"), None, None),
        P(),
        P(("own", "dom"), None),
        P(("own", "dom"), None),
        P(None, ("own", "dom"), None),
        P(("own", "dom")),
        P("own", "dom"),
        P("own", "dom"),
    )
    return jax.shard_map(
        shards,
        mesh=mesh,
        in_specs=placed,
        out_specs=(P(("own", "dom"), None, None), P("own", "dom")),
        check_vma=False,
    )
```

```python
import jax
import jax.numpy as jnp
from jax import lax
from jax.experimental import pallas as pl
from jax.experimental.pallas import tpu as pltpu
from jax.sharding import PartitionSpec as P

TILE = 64
TCOLS = 32
TILES_DEV = 2
FIELDS = 6
SWEEPS = 4
KAPPA = 0.08
NEED = 32
NPS = 1024
LANES = 128
GROUPS = NPS // LANES
N_OWN = 8
N_DOM = 64
BAND = TILES_DEV * N_DOM
CORES = 2
MSG = 12
QUARTERS = 3
NOTHING = 0xFFFF
CHUNK = 256
PER_CHUNK = CHUNK // LANES
CHUNKS = NPS // CHUNK
FIELD_BITS = 10
ABSENT = (CHUNKS - 1) * FIELD_BITS << 16
LIST = 8 * FIELD_BITS
FX_STEP = 2.0**-16
FY_TOP = 65535.0


SMALL = pltpu.CompilerParams(vmem_limit_bytes=8 * 2**20)


def iota(shape, dim):
    return lax.broadcasted_iota(jnp.int32, shape, dim)


def storm_field(place_ref, track_ref, background_ref, out_ref, rows_ref):
    field = iota((8, LANES), 0)
    lane = iota((8, LANES), 1)
    late = field >= 3
    centre_x, centre_y, deficit, max_radius, exponent = (
        jnp.where(late, track_ref[1, i], track_ref[0, i]) for i in range(5)
    )
    kind = jnp.where(late, field - 3, field)
    strength = exponent * deficit
    left = lane < TILE

    def one_field(tile, chunk):
        tile_index = place_ref[0] * TILES_DEV + tile
        north = (tile_index // TCOLS * TILE + 2 * chunk + lane // TILE).astype(jnp.float32)
        east = (tile_index % TCOLS * TILE + lane % TILE).astype(jnp.float32)
        offset_x = east - centre_x
        offset_y = north - centre_y
        radius = jnp.sqrt(offset_x * offset_x + offset_y * offset_y + 1.0)
        ratio = jnp.exp(exponent * jnp.log(max_radius / radius))
        decay = jnp.exp(-ratio)
        speed = jnp.sqrt(strength * ratio * decay)
        wind = speed * jnp.where(kind == 0, -offset_y, offset_x) / radius
        storm = jnp.where(kind == 2, -deficit * (1.0 - decay), wind)
        piece = background_ref[:, tile, pl.ds(pl.multiple_of(chunk * LANES, LANES), LANES)]
        return piece.astype(jnp.float32) + storm[:FIELDS]

    def step(chunk, carry):
        first = one_field(0, chunk)
        second = one_field(1, chunk)
        even = jnp.where(left[:FIELDS], first, pltpu.roll(second, TILE, 1))
        odd = jnp.where(left[:FIELDS], pltpu.roll(first, TILE, 1), second)
        rows_ref[pl.ds(2 * chunk, FIELDS, stride=TILE), :] = even
        rows_ref[pl.ds(2 * chunk + 1, FIELDS, stride=TILE), :] = odd
        return carry

    lax.fori_loop(0, TILE // 2, step, 0, unroll=8)
    out_ref[...] = rows_ref[...].astype(jnp.bfloat16)


def column_code(fraction):
    scaled = fraction * 32768.0
    whole = jnp.floor(scaled)
    code = 2.0 * whole + jnp.where(scaled > whole, 1.0, 0.0)
    return jnp.minimum(code, 65534.0).astype(jnp.int32)


def row_code(fraction):
    return jnp.floor(fraction * FY_TOP + 0.5).astype(jnp.int32)


def prepare_kernel(
    place_ref,
    track_ref,
    need_ref,
    count_ref,
    background_ref,
    cells_ref,
    fracs_ref,
    ehead_ref,
    etail_ref,
    bhead_ref,
    btail_ref,
    tiles_ref,
    out_ref,
    first_ref,
    last_ref,
    rows_ref,
    stage_ref,
):
    storm_field(place_ref, track_ref, background_ref, tiles_ref, rows_ref)
    for g in range(GROUPS):
        span = slice(g * LANES, (g + 1) * LANES)
        word = cells_ref[:, span] | (column_code(fracs_ref[0, :, span]) << 16)
        stage_ref[pl.ds(g, NEED, stride=MSG), :] = word
    for g in range(GROUPS // 2):
        low = row_code(fracs_ref[1, :, g * LANES : (g + 1) * LANES])
        high = row_code(fracs_ref[1, :, NPS // 2 + g * LANES : NPS // 2 + (g + 1) * LANES])
        stage_ref[pl.ds(GROUPS + g, NEED, stride=MSG), :] = low | (high << 16)
    first_ref[0:1, :] = ehead_ref[0:1, :]
    first_ref[1:2, :] = bhead_ref[0:1, :]
    last_ref[0:1, :] = etail_ref[7:8, :]
    last_ref[1:2, :] = btail_ref[7:8, :]
    first_ref[2:8, :] = jnp.zeros((6, LANES), jnp.float32)
    last_ref[2:8, :] = jnp.zeros((6, LANES), jnp.float32)
    position = iota((4, LANES), 0) * LANES + iota((4, LANES), 1)
    nothing = jnp.full((4, LANES), -1, jnp.int32)

    def clear(d, carry):
        out_ref[d, 0] = nothing
        return carry

    lax.fori_loop(0, N_DOM, clear, 0, unroll=8)

    def ask(s, carry):
        tile = need_ref[0, s]
        count = count_ref[s]
        holder = tile % BAND // TILES_DEV
        start = (tile // BAND * TILES_DEV + tile % TILES_DEV) * (TILE * TILE)
        at = pl.multiple_of(s * MSG, 4)
        for h in range(2):
            words = stage_ref[pl.ds(at + 4 * h, 4), :] | start
            out_ref[holder, h] = jnp.where(position + h * (NPS // 2) < count, words, nothing)
        out_ref[holder, 2] = stage_ref[pl.ds(at + 8, 4), :]
        return carry

    lax.fori_loop(0, NEED, ask, 0, unroll=4)


def prepare(place, storm_track, need_tiles, slot_count, background, node_cells, node_fracs, elevation, bed_level):
    last = elevation.shape[0] // 8 - 1
    head = pl.BlockSpec((8, LANES), lambda i: (0, 0))
    tail = pl.BlockSpec((8, LANES), lambda i: (last, 0))
    vmem = pl.BlockSpec(memory_space=pltpu.VMEM)
    rows = FIELDS * TILE
    return pl.pallas_call(
        prepare_kernel,
        grid=(1,),
        out_shape=(
            jax.ShapeDtypeStruct((rows, LANES), jnp.bfloat16),
            jax.ShapeDtypeStruct((N_DOM, QUARTERS, 4, LANES), jnp.int32),
            jax.ShapeDtypeStruct((8, LANES), jnp.float32),
            jax.ShapeDtypeStruct((8, LANES), jnp.float32),
        ),
        in_specs=[pl.BlockSpec(memory_space=pltpu.SMEM)] * 4 + [vmem] * 3 + [head, tail, head, tail],
        out_specs=(vmem,) * 4,
        scratch_shapes=[
            pltpu.VMEM((rows, LANES), jnp.float32),
            pltpu.VMEM((NEED * MSG, LANES), jnp.int32),
        ],
    )(
        place,
        storm_track,
        need_tiles,
        slot_count,
        background.transpose(1, 0, 2),
        node_cells,
        node_fracs,
        elevation,
        elevation,
        bed_level,
        bed_level,
    )


SLOT_ROWS = FIELDS * GROUPS * 8
HALF = FIELDS // 2


def interpolate_kernel(
    place_ref,
    header_ref,
    message_ref,
    near0,
    near1,
    near2,
    near3,
    far_ref,
    out_ref,
    tiles_ref,
    x_ref,
    y_ref,
    part_ref,
    list_ref,
):
    own = place_ref[0] // N_DOM

    def keep(band, pair):
        tiles_ref[2 * band] = pair
        tiles_ref[2 * band + 1] = pltpu.roll(pair, TILE, 1)

    for shift, ref in enumerate((near0, near1, near2, near3)):
        band = (own + N_OWN - CORES * shift) % N_OWN
        keep(band, ref[...])
        keep(band + 1 - 2 * (band % CORES), far_ref[shift])

    packed = jnp.int32(0)
    for s in range(N_DOM):
        shift = header_ref[s] >> 16
        list_ref[shift * 8 + (lax.shift_right_logical(packed, shift) & (2**FIELD_BITS - 1))] = s
        packed = packed + (1 << shift)
    counts = [packed >> i * FIELD_BITS & (2**FIELD_BITS - 1) for i in range(CHUNKS - 1)]
    spot = iota((TILE, LANES), 0).astype(jnp.float32)

    def add_up(i, slot):
        values = []
        for f in range(FIELDS):
            at = i * SLOT_ROWS + f * 64
            pieces = [part_ref[pl.ds(at + j, GROUPS, stride=8), :] for j in range(8)]
            while len(pieces) > 1:
                pieces = [a + b for a, b in zip(pieces[::2], pieces[1::2])]
            values.append(pieces[0])
        out_ref[slot] = jnp.concatenate(values, axis=0).astype(jnp.bfloat16)

    def hat(ref, at):
        return jnp.maximum(1.0 - jnp.abs(spot - ref[at : at + 1, :]), 0.0)

    def decode(i, s):
        pair = message_ref[s, 2]
        for h in range(2):
            word = message_ref[s, h]
            column = lax.shift_right_logical(word, 16)
            row_part = lax.shift_right_logical(pair, 16) if h else pair & 0xFFFF
            row = ((word >> 6) & (TILE - 1)).astype(jnp.float32) + row_part.astype(jnp.float32) * (1.0 / FY_TOP)
            here = slice(8 * i + 4 * h, 8 * i + 4 * h + 4)
            x_ref[here, :] = (word & (TILE - 1)).astype(jnp.float32) + column.astype(jnp.float32) * FX_STEP
            y_ref[here, :] = jnp.where(column == NOTHING, -4.0, row)

    def two_slots(slots, before, live):
        for i in range(2):
            add_up(i, before[i])
        for i in range(2):
            decode(i, slots[i])
        tiles = [tiles_ref[header_ref[s] & 0xFFFF, :, 0:TILE] for s in slots]
        for c in range(live):
            for i in range(2):
                groups = range(c * PER_CHUNK, (c + 1) * PER_CHUNK)
                columns = jnp.concatenate([hat(x_ref, 8 * i + g).astype(jnp.bfloat16) for g in groups], axis=1)
                rows = jnp.concatenate([hat(y_ref, 8 * i + g) for g in groups], axis=1)
                for f in range(FIELDS):
                    if f % HALF == 0:
                        part = tiles[i][f * TILE : (f + HALF) * TILE]
                        spread = jnp.dot(part, columns, preferred_element_type=jnp.float32)
                    weighed = spread[f % HALF * TILE : (f % HALF + 1) * TILE] * rows
                    total = jnp.sum(weighed.reshape(TILE // 8, 8, CHUNK), axis=0)
                    for j, g in enumerate(groups):
                        at = i * SLOT_ROWS + (f * GROUPS + g) * 8
                        part_ref[at : at + 8, :] = total[:, j * LANES : (j + 1) * LANES]
        dead = (CHUNKS - live) * PER_CHUNK * 8
        if dead:
            for i in range(2):
                for f in range(FIELDS):
                    at = i * SLOT_ROWS + (f + 1) * GROUPS * 8 - dead
                    part_ref[at : at + dead, :] = jnp.zeros((dead, LANES), jnp.float32)

    before = (jnp.int32(-1), jnp.int32(-1))
    for i, n in enumerate(counts):

        @pl.when(n > 0)
        def _():
            list_ref[i * LIST + n] = list_ref[i * LIST + n - 1]

        def step(p, before):
            slots = (list_ref[i * LIST + 2 * p], list_ref[i * LIST + 2 * p + 1])
            two_slots(slots, tuple(jnp.where(b < 0, s, b) for b, s in zip(before, slots)), i + 2)
            return slots

        before = lax.fori_loop(0, (n + 1) // 2, step, before)
    for i in range(2):
        add_up(i, jnp.maximum(before[i], 0))


def interpolate(place, header, message, near, far):
    return pl.pallas_call(
        interpolate_kernel,
        out_shape=jax.ShapeDtypeStruct((N_DOM, FIELDS * GROUPS, LANES), jnp.bfloat16),
        in_specs=[pl.BlockSpec(memory_space=pltpu.SMEM)] * 2 + [pl.BlockSpec(memory_space=pltpu.VMEM)] * 6,
        out_specs=pl.BlockSpec(memory_space=pltpu.VMEM),
        scratch_shapes=[
            pltpu.VMEM((N_OWN * TILES_DEV, FIELDS * TILE, LANES), jnp.bfloat16),
            pltpu.VMEM((2 * GROUPS, LANES), jnp.float32),
            pltpu.VMEM((2 * GROUPS, LANES), jnp.float32),
            pltpu.VMEM((2 * SLOT_ROWS, LANES), jnp.float32),
            pltpu.SMEM((CHUNKS * LIST,), jnp.int32),
        ],
        compiler_params=SMALL,
    )(place, header, message, *near, far)


def following(x, lane):
    moved = pltpu.roll(x, LANES - 1, 1)
    return jnp.where(lane == LANES - 1, pltpu.roll(moved, x.shape[0] - 1, 0), moved)


def preceding(x, lane):
    moved = pltpu.roll(x, 1, 1)
    return jnp.where(lane == 0, pltpu.roll(moved, 1, 0), moved)


def flux_sweeps(place_ref, before_ref, after_ref, elevation_ref, bed_ref, out_ref):
    rows = elevation_ref.shape[0]
    lane8 = iota((8, LANES), 1)
    row8 = iota((8, LANES), 0)

    def ends(which):
        before = before_ref[which : which + 1, :]
        after = after_ref[which : which + 1, :]
        top = jnp.where((row8 == 7) & (lane8 >= LANES - SWEEPS), before, 0.0)
        bottom = jnp.where((row8 == 0) & (lane8 < SWEEPS), after, 0.0)
        return top, bottom

    surface_top, surface_bottom = ends(0)
    bed_top, bed_bottom = ends(1)
    surface = jnp.concatenate([surface_top, elevation_ref[...], surface_bottom], axis=0)
    bed = jnp.concatenate([bed_top, bed_ref[...], bed_bottom], axis=0)
    lane = iota(surface.shape, 1)
    node = iota(surface.shape, 0) * LANES + lane
    dom = place_ref[0] % N_DOM
    first_wall = jnp.where(dom == 0, 8 * LANES - 1, -1)
    last_wall = jnp.where(dom == N_DOM - 1, (8 + rows) * LANES - 1, -1)
    open_face = jnp.where((node == first_wall) | (node == last_wall), 0.0, KAPPA)
    for _ in range(SWEEPS):
        wet = jnp.maximum(surface - bed, 0.0)
        drop = surface - following(surface, lane)
        upwind = jnp.where(drop >= 0.0, wet, following(wet, lane))
        flux = open_face * upwind * drop
        surface = surface - (flux - preceding(flux, lane))
    out_ref[...] = surface[8 : 8 + rows]


SLOTS8 = 8


def finish_kernel(
    place_ref,
    need_ref,
    returned_ref,
    before_ref,
    after_ref,
    elevation_ref,
    bed_ref,
    forcing_ref,
    surge_ref,
    surface_ref,
    stage_ref,
):
    rows = FIELDS * GROUPS
    flux_sweeps(place_ref, before_ref, after_ref, elevation_ref, bed_ref, surface_ref)

    def eight_slots(b, carry):
        for i in range(SLOTS8):
            s = b * SLOTS8 + i
            block = returned_ref[need_ref[0, s] % BAND // TILES_DEV].astype(jnp.float32)
            stage_ref[i * rows : (i + 1) * rows, :] = block
            here = pl.ds(pl.multiple_of(s * GROUPS, GROUPS), GROUPS)
            surface = surface_ref[here, :]
            wet = jnp.minimum(jnp.maximum(surface - bed_ref[here, :], 0.0), 1.0)
            surge_ref[here, :] = surface - 0.5 * block[rows - GROUPS :] * wet
        slots = pl.ds(pl.multiple_of(b * SLOTS8, SLOTS8), SLOTS8)
        for f in range(FIELDS):
            for g in range(GROUPS):
                piece = stage_ref[pl.ds(f * GROUPS + g, SLOTS8, stride=rows), :]
                forcing_ref[f, slots, g * LANES : (g + 1) * LANES] = piece.astype(jnp.bfloat16)
        return carry

    lax.fori_loop(0, NEED // SLOTS8, eight_slots, 0)


def finish(place, need_tiles, returned, before, after, elevation, bed_level):
    def whole(shape):
        return pl.BlockSpec(shape, lambda i, *refs: (0,) * len(shape))

    forcing = (FIELDS, NEED, NPS)
    return pl.pallas_call(
        finish_kernel,
        out_shape=(
            jax.ShapeDtypeStruct(forcing, jnp.bfloat16),
            jax.ShapeDtypeStruct(elevation.shape, jnp.float32),
        ),
        grid_spec=pltpu.PrefetchScalarGridSpec(
            num_scalar_prefetch=2,
            grid=(1,),
            in_specs=[
                whole(returned.shape),
                whole(before.shape),
                whole(after.shape),
                whole(elevation.shape),
                whole(elevation.shape),
            ],
            out_specs=(whole(forcing), whole(elevation.shape)),
            scratch_shapes=[
                pltpu.VMEM(elevation.shape, jnp.float32),
                pltpu.VMEM((SLOTS8 * FIELDS * GROUPS, LANES), jnp.float32),
            ],
        ),
        compiler_params=SMALL,
    )(place, need_tiles, returned, before, after, elevation, bed_level)


def exchange(blocks, axis):
    return lax.all_to_all(blocks, axis, split_axis=0, concat_axis=0, tiled=True)


def shards(
    background, storm_track, need_tiles, node_cells, node_fracs, slot_count, elevation, bed_level
):
    place = (lax.axis_index("own") * N_DOM + lax.axis_index("dom"))[None].astype(jnp.int32)
    elevation = elevation.reshape(-1, LANES)
    bed_level = bed_level.reshape(-1, LANES)
    tiles, question, first, last = prepare(
        place, storm_track, need_tiles, slot_count, background, node_cells, node_fracs, elevation, bed_level
    )
    near = [tiles]
    for shift in range(CORES, N_OWN, CORES):
        near.append(lax.ppermute(tiles, "own", [(i, (i + shift) % N_OWN) for i in range(N_OWN)]))
    message = exchange(question, "dom")
    far = lax.ppermute(jnp.stack(near), "own", [(i, i ^ 1) for i in range(N_OWN)])
    before = lax.ppermute(last, "dom", [(i, i + 1) for i in range(N_DOM - 1)])
    after = lax.ppermute(first, "dom", [(i + 1, i) for i in range(N_DOM - 1)])
    start, middle, late = message[:, 0, 0, 0], message[:, 1, 0, 0], message[:, 1, 2, 0]
    live = FIELD_BITS * ((middle >> 16 != -1).astype(jnp.int32) + (late >> 16 != -1).astype(jnp.int32))
    header = jnp.where(start >> 16 == -1, ABSENT, (start >> 12 & 15) | live << 16)
    header, before, after = lax.optimization_barrier((header, before, after))
    answers = interpolate(place, header, message, near, far)
    returned = exchange(answers, "dom")
    forcing, surge = finish(place, need_tiles, returned, before, after, elevation, bed_level)
    return forcing.transpose(1, 0, 2), surge.reshape(1, -1)


def solution(mesh):
    placed = (
        P(("own", "dom"), None, None),
        P(),
        P(("own", "dom"), None),
        P(("own", "dom"), None),
        P(None, ("own", "dom"), None),
        P(("own", "dom")),
        P("own", "dom"),
        P("own", "dom"),
    )
    return jax.shard_map(
        shards,
        mesh=mesh,
        in_specs=placed,
        out_specs=(P(("own", "dom"), None, None), P("own", "dom")),
        check_vma=False,
    )
```

```python
import jax
import jax.numpy as jnp
from jax import lax
from jax.experimental import pallas as pl
from jax.experimental.pallas import tpu as pltpu
from jax.sharding import PartitionSpec as P

TILE = 64
TCOLS = 32
TILES_DEV = 2
FIELDS = 6
SWEEPS = 4
KAPPA = 0.08
NEED = 32
NPS = 1024
LANES = 128
GROUPS = NPS // LANES
N_OWN = 8
N_DOM = 64
BAND = TILES_DEV * N_DOM
CORES = 2
MSG = 16
CHUNK = 256
PER_CHUNK = CHUNK // LANES
CHUNKS = NPS // CHUNK
FIELD_BITS = 10
ABSENT = (CHUNKS - 1) * FIELD_BITS << 16
LIST = 8 * FIELD_BITS
DEAD_CELL = 0xFFC0
EDGE_SCALE = 2.0**29
FX_STEP = 2.0**-16
FY_TOP = 65535.0


SMALL = pltpu.CompilerParams(vmem_limit_bytes=8 * 2**20)


def iota(shape, dim):
    return lax.broadcasted_iota(jnp.int32, shape, dim)


def storm_field(place_ref, track_ref, background_ref, out_ref, rows_ref):
    field = iota((8, LANES), 0)
    lane = iota((8, LANES), 1)
    late = field >= 3
    centre_x, centre_y, deficit, max_radius, exponent = (
        jnp.where(late, track_ref[1, i], track_ref[0, i]) for i in range(5)
    )
    kind = jnp.where(late, field - 3, field)
    strength = exponent * deficit
    left = lane < TILE

    def one_field(tile, chunk):
        tile_index = place_ref[0] * TILES_DEV + tile
        north = (tile_index // TCOLS * TILE + 2 * chunk + lane // TILE).astype(jnp.float32)
        east = (tile_index % TCOLS * TILE + lane % TILE).astype(jnp.float32)
        offset_x = east - centre_x
        offset_y = north - centre_y
        radius = jnp.sqrt(offset_x * offset_x + offset_y * offset_y + 1.0)
        ratio = jnp.exp(exponent * jnp.log(max_radius / radius))
        decay = jnp.exp(-ratio)
        speed = jnp.sqrt(strength * ratio * decay)
        wind = speed * jnp.where(kind == 0, -offset_y, offset_x) / radius
        storm = jnp.where(kind == 2, -deficit * (1.0 - decay), wind)
        piece = background_ref[:, tile, pl.ds(pl.multiple_of(chunk * LANES, LANES), LANES)]
        return piece.astype(jnp.float32) + storm[:FIELDS]

    def step(chunk, carry):
        first = one_field(0, chunk)
        second = one_field(1, chunk)
        even = jnp.where(left[:FIELDS], first, pltpu.roll(second, TILE, 1))
        odd = jnp.where(left[:FIELDS], pltpu.roll(first, TILE, 1), second)
        rows_ref[pl.ds(2 * chunk, FIELDS, stride=TILE), :] = even
        rows_ref[pl.ds(2 * chunk + 1, FIELDS, stride=TILE), :] = odd
        return carry

    lax.fori_loop(0, TILE // 2, step, 0, unroll=8)
    out_ref[...] = rows_ref[...].astype(jnp.bfloat16)


def column_code(fraction):
    scaled = fraction * 32768.0
    whole = jnp.floor(scaled)
    code = 2.0 * whole + jnp.where(scaled > whole, 1.0, 0.0)
    return jnp.minimum(code, 65535.0).astype(jnp.int32)


def row_code(fraction):
    return jnp.floor(fraction * FY_TOP + 0.5).astype(jnp.int32)


def edge_code(value):
    return jnp.floor(value * EDGE_SCALE + 0.5).astype(jnp.int32)


def prepare_kernel(
    place_ref,
    track_ref,
    need_ref,
    count_ref,
    background_ref,
    cells_ref,
    fracs_ref,
    ehead_ref,
    etail_ref,
    bhead_ref,
    btail_ref,
    tiles_ref,
    out_ref,
    rows_ref,
    stage_ref,
):
    storm_field(place_ref, track_ref, background_ref, tiles_ref, rows_ref)
    for g in range(GROUPS):
        span = slice(g * LANES, (g + 1) * LANES)
        word = cells_ref[:, span] | (column_code(fracs_ref[0, :, span]) << 16)
        stage_ref[pl.ds(g, NEED, stride=MSG), :] = word
    for g in range(GROUPS // 2):
        low = row_code(fracs_ref[1, :, g * LANES : (g + 1) * LANES])
        high = row_code(fracs_ref[1, :, NPS // 2 + g * LANES : NPS // 2 + (g + 1) * LANES])
        stage_ref[pl.ds(GROUPS + g, NEED, stride=MSG), :] = low | (high << 16)
    row = iota((8, LANES), 0)
    lane = iota((8, LANES), 1)
    position = row * LANES + lane
    surface = jnp.where(lane < SWEEPS, ehead_ref[0:1, :], etail_ref[7:8, :])
    bed = jnp.where(lane < SWEEPS, bhead_ref[0:1, :], btail_ref[7:8, :])
    plain = jnp.where(row == 5, edge_code(surface), jnp.where(row == 6, edge_code(bed), ABSENT))

    def clear(d, carry):
        out_ref[d, 8:16, :] = plain
        return carry

    lax.fori_loop(0, N_DOM, clear, 0, unroll=8)

    def place(s, carry):
        tile = need_ref[0, s]
        count = count_ref[s]
        holder = tile % BAND // TILES_DEV
        live = jnp.maximum((count + CHUNK - 1) // CHUNK, 2)
        header = (tile // BAND * TILES_DEV + tile % TILES_DEV) | ((live - 2) * FIELD_BITS << 16)
        start = pl.multiple_of(s * MSG, MSG)
        out_ref[holder, 0:8, :] = jnp.where(position < count, stage_ref[pl.ds(start, 8), :], DEAD_CELL)
        out_ref[holder, 8:16, :] = jnp.where(
            row < 4, stage_ref[pl.ds(start + 8, 8), :], jnp.where(row == 4, header, plain)
        )
        return carry

    lax.fori_loop(0, NEED, place, 0, unroll=4)


def prepare(place, storm_track, need_tiles, slot_count, background, node_cells, node_fracs, elevation, bed_level):
    last = elevation.shape[0] // 8 - 1
    head = pl.BlockSpec((8, LANES), lambda i: (0, 0))
    tail = pl.BlockSpec((8, LANES), lambda i: (last, 0))
    vmem = pl.BlockSpec(memory_space=pltpu.VMEM)
    rows = FIELDS * TILE
    return pl.pallas_call(
        prepare_kernel,
        grid=(1,),
        out_shape=(
            jax.ShapeDtypeStruct((rows, LANES), jnp.bfloat16),
            jax.ShapeDtypeStruct((N_DOM, MSG, LANES), jnp.int32),
        ),
        in_specs=[pl.BlockSpec(memory_space=pltpu.SMEM)] * 4 + [vmem] * 3 + [head, tail, head, tail],
        out_specs=(vmem, vmem),
        scratch_shapes=[
            pltpu.VMEM((rows, LANES), jnp.float32),
            pltpu.VMEM((NEED * MSG, LANES), jnp.int32),
        ],
    )(
        place,
        storm_track,
        need_tiles,
        slot_count,
        background.transpose(1, 0, 2),
        node_cells,
        node_fracs,
        elevation,
        elevation,
        bed_level,
        bed_level,
    )


SLOT_ROWS = FIELDS * GROUPS * 8
HALF = FIELDS // 2


def interpolate_kernel(
    place_ref,
    message_ref,
    near0,
    near1,
    near2,
    near3,
    far_ref,
    out_ref,
    tiles_ref,
    x_ref,
    y_ref,
    part_ref,
    list_ref,
    header_ref,
    sem,
):
    headers = pltpu.make_async_copy(message_ref.at[:, 12:13, :], header_ref, sem)
    headers.start()
    own = place_ref[0] // N_DOM

    def keep(band, pair):
        tiles_ref[2 * band] = pair
        tiles_ref[2 * band + 1] = pltpu.roll(pair, TILE, 1)

    for shift, ref in enumerate((near0, near1, near2, near3)):
        band = (own + N_OWN - CORES * shift) % N_OWN
        keep(band, ref[...])
        keep(band + 1 - 2 * (band % CORES), far_ref[shift])

    headers.wait()
    packed = jnp.int32(0)
    for s in range(N_DOM):
        shift = header_ref[s, 0, 0] >> 16
        list_ref[shift * 8 + (lax.shift_right_logical(packed, shift) & (2**FIELD_BITS - 1))] = s
        packed = packed + (1 << shift)
    counts = [packed >> i * FIELD_BITS & (2**FIELD_BITS - 1) for i in range(CHUNKS - 1)]
    spot = iota((TILE, LANES), 0).astype(jnp.float32)

    def add_up(i, slot):
        values = []
        for f in range(FIELDS):
            at = i * SLOT_ROWS + f * 64
            pieces = [part_ref[pl.ds(at + j, GROUPS, stride=8), :] for j in range(8)]
            while len(pieces) > 1:
                pieces = [a + b for a, b in zip(pieces[::2], pieces[1::2])]
            values.append(pieces[0])
        out_ref[slot] = jnp.concatenate(values, axis=0).astype(jnp.bfloat16)

    def hat(ref, at):
        return jnp.maximum(1.0 - jnp.abs(spot - ref[at : at + 1, :]), 0.0)

    def decode(i, s):
        word = message_ref[s, 0:8, :]
        pair = message_ref[s, 8:16, :]
        cell = word & 0xFFFF
        row = (cell // TILE).astype(jnp.float32)
        low = (pair[0:4] & 0xFFFF).astype(jnp.float32)
        high = lax.shift_right_logical(pair[0:4], 16).astype(jnp.float32)
        x_ref[8 * i : 8 * i + 8, :] = (cell & (TILE - 1)).astype(jnp.float32) + lax.shift_right_logical(
            word, 16
        ).astype(jnp.float32) * FX_STEP
        y_ref[8 * i : 8 * i + 4, :] = row[0:4] + low * (1.0 / FY_TOP)
        y_ref[8 * i + 4 : 8 * i + 8, :] = row[4:8] + high * (1.0 / FY_TOP)

    def two_slots(slots, before, live):
        for i in range(2):
            add_up(i, before[i])
        for i in range(2):
            decode(i, slots[i])
        tiles = [tiles_ref[header_ref[s, 0, 0] & 0xFFFF, :, 0:TILE] for s in slots]
        for c in range(live):
            for i in range(2):
                groups = range(c * PER_CHUNK, (c + 1) * PER_CHUNK)
                columns = jnp.concatenate([hat(x_ref, 8 * i + g).astype(jnp.bfloat16) for g in groups], axis=1)
                rows = jnp.concatenate([hat(y_ref, 8 * i + g) for g in groups], axis=1)
                for f in range(FIELDS):
                    if f % HALF == 0:
                        part = tiles[i][f * TILE : (f + HALF) * TILE]
                        spread = jnp.dot(part, columns, preferred_element_type=jnp.float32)
                    weighed = spread[f % HALF * TILE : (f % HALF + 1) * TILE] * rows
                    total = jnp.sum(weighed.reshape(TILE // 8, 8, CHUNK), axis=0)
                    for j, g in enumerate(groups):
                        at = i * SLOT_ROWS + (f * GROUPS + g) * 8
                        part_ref[at : at + 8, :] = total[:, j * LANES : (j + 1) * LANES]
        dead = (CHUNKS - live) * PER_CHUNK * 8
        if dead:
            for i in range(2):
                for f in range(FIELDS):
                    at = i * SLOT_ROWS + (f + 1) * GROUPS * 8 - dead
                    part_ref[at : at + dead, :] = jnp.zeros((dead, LANES), jnp.float32)

    before = (jnp.int32(-1), jnp.int32(-1))
    for i, n in enumerate(counts):

        @pl.when(n > 0)
        def _():
            list_ref[i * LIST + n] = list_ref[i * LIST + n - 1]

        def step(p, before):
            slots = (list_ref[i * LIST + 2 * p], list_ref[i * LIST + 2 * p + 1])
            two_slots(slots, tuple(jnp.where(b < 0, s, b) for b, s in zip(before, slots)), i + 2)
            return slots

        before = lax.fori_loop(0, (n + 1) // 2, step, before)
    for i in range(2):
        add_up(i, jnp.maximum(before[i], 0))


def interpolate(place, message, near, far):
    return pl.pallas_call(
        interpolate_kernel,
        out_shape=jax.ShapeDtypeStruct((N_DOM, FIELDS * GROUPS, LANES), jnp.bfloat16),
        in_specs=[pl.BlockSpec(memory_space=pltpu.SMEM)] + [pl.BlockSpec(memory_space=pltpu.VMEM)] * 6,
        out_specs=pl.BlockSpec(memory_space=pltpu.VMEM),
        scratch_shapes=[
            pltpu.VMEM((N_OWN * TILES_DEV, FIELDS * TILE, LANES), jnp.bfloat16),
            pltpu.VMEM((2 * GROUPS, LANES), jnp.float32),
            pltpu.VMEM((2 * GROUPS, LANES), jnp.float32),
            pltpu.VMEM((2 * SLOT_ROWS, LANES), jnp.float32),
            pltpu.SMEM((CHUNKS * LIST,), jnp.int32),
            pltpu.SMEM((N_DOM, 1, LANES), jnp.int32),
            pltpu.SemaphoreType.DMA,
        ],
        compiler_params=SMALL,
    )(place, message, *near, far)


def following(x, lane):
    moved = pltpu.roll(x, LANES - 1, 1)
    return jnp.where(lane == LANES - 1, pltpu.roll(moved, x.shape[0] - 1, 0), moved)


def preceding(x, lane):
    moved = pltpu.roll(x, 1, 1)
    return jnp.where(lane == 0, pltpu.roll(moved, 1, 0), moved)


def flux_sweeps(place_ref, before_ref, after_ref, elevation_ref, bed_ref, out_ref):
    rows = elevation_ref.shape[0]
    lane8 = iota((8, LANES), 1)
    row8 = iota((8, LANES), 0)

    def ends(which):
        before = before_ref[0, which : which + 1, :].astype(jnp.float32) * (1.0 / EDGE_SCALE)
        after = after_ref[0, which : which + 1, :].astype(jnp.float32) * (1.0 / EDGE_SCALE)
        top = jnp.where((row8 == 7) & (lane8 >= LANES - SWEEPS), before, 0.0)
        bottom = jnp.where((row8 == 0) & (lane8 < SWEEPS), after, 0.0)
        return top, bottom

    surface_top, surface_bottom = ends(5)
    bed_top, bed_bottom = ends(6)
    surface = jnp.concatenate([surface_top, elevation_ref[...], surface_bottom], axis=0)
    bed = jnp.concatenate([bed_top, bed_ref[...], bed_bottom], axis=0)
    lane = iota(surface.shape, 1)
    node = iota(surface.shape, 0) * LANES + lane
    dom = place_ref[0] % N_DOM
    first_wall = jnp.where(dom == 0, 8 * LANES - 1, -1)
    last_wall = jnp.where(dom == N_DOM - 1, (8 + rows) * LANES - 1, -1)
    open_face = jnp.where((node == first_wall) | (node == last_wall), 0.0, KAPPA)
    for _ in range(SWEEPS):
        wet = jnp.maximum(surface - bed, 0.0)
        drop = surface - following(surface, lane)
        upwind = jnp.where(drop >= 0.0, wet, following(wet, lane))
        flux = open_face * upwind * drop
        surface = surface - (flux - preceding(flux, lane))
    out_ref[...] = surface[8 : 8 + rows]


SLOTS8 = 8


def finish_kernel(
    place_ref,
    need_ref,
    returned_ref,
    before_ref,
    after_ref,
    elevation_ref,
    bed_ref,
    forcing_ref,
    surge_ref,
    surface_ref,
    stage_ref,
):
    rows = FIELDS * GROUPS
    flux_sweeps(place_ref, before_ref, after_ref, elevation_ref, bed_ref, surface_ref)

    def eight_slots(b, carry):
        for i in range(SLOTS8):
            s = b * SLOTS8 + i
            block = returned_ref[need_ref[0, s] % BAND // TILES_DEV].astype(jnp.float32)
            stage_ref[i * rows : (i + 1) * rows, :] = block
            here = pl.ds(pl.multiple_of(s * GROUPS, GROUPS), GROUPS)
            surface = surface_ref[here, :]
            wet = jnp.minimum(jnp.maximum(surface - bed_ref[here, :], 0.0), 1.0)
            surge_ref[here, :] = surface - 0.5 * block[rows - GROUPS :] * wet
        slots = pl.ds(pl.multiple_of(b * SLOTS8, SLOTS8), SLOTS8)
        for f in range(FIELDS):
            for g in range(GROUPS):
                piece = stage_ref[pl.ds(f * GROUPS + g, SLOTS8, stride=rows), :]
                forcing_ref[f, slots, g * LANES : (g + 1) * LANES] = piece.astype(jnp.bfloat16)
        return carry

    lax.fori_loop(0, NEED // SLOTS8, eight_slots, 0)


def finish(place, need_tiles, returned, message, elevation, bed_level):
    def whole(shape):
        return pl.BlockSpec(shape, lambda i, *refs: (0,) * len(shape))

    def neighbour(step):
        return pl.BlockSpec((1, 8, LANES), lambda i, place_ref, need_ref: ((place_ref[0] + step) % N_DOM, 1, 0))

    forcing = (FIELDS, NEED, NPS)
    return pl.pallas_call(
        finish_kernel,
        out_shape=(
            jax.ShapeDtypeStruct(forcing, jnp.bfloat16),
            jax.ShapeDtypeStruct(elevation.shape, jnp.float32),
        ),
        grid_spec=pltpu.PrefetchScalarGridSpec(
            num_scalar_prefetch=2,
            grid=(1,),
            in_specs=[
                whole(returned.shape),
                neighbour(N_DOM - 1),
                neighbour(1),
                whole(elevation.shape),
                whole(elevation.shape),
            ],
            out_specs=(whole(forcing), whole(elevation.shape)),
            scratch_shapes=[
                pltpu.VMEM(elevation.shape, jnp.float32),
                pltpu.VMEM((SLOTS8 * FIELDS * GROUPS, LANES), jnp.float32),
            ],
        ),
        compiler_params=SMALL,
    )(place, need_tiles, returned, message, message, elevation, bed_level)


def exchange(blocks, axis):
    return lax.all_to_all(blocks, axis, split_axis=0, concat_axis=0, tiled=True)


def shards(
    background, storm_track, need_tiles, node_cells, node_fracs, slot_count, elevation, bed_level
):
    place = (lax.axis_index("own") * N_DOM + lax.axis_index("dom"))[None].astype(jnp.int32)
    elevation = elevation.reshape(-1, LANES)
    bed_level = bed_level.reshape(-1, LANES)
    tiles, question = prepare(
        place, storm_track, need_tiles, slot_count, background, node_cells, node_fracs, elevation, bed_level
    )
    near = [tiles]
    for shift in range(CORES, N_OWN, CORES):
        near.append(lax.ppermute(tiles, "own", [(i, (i + shift) % N_OWN) for i in range(N_OWN)]))
    message = exchange(question, "dom")
    far = lax.ppermute(jnp.stack(near), "own", [(i, i ^ 1) for i in range(N_OWN)])
    answers = interpolate(place, message, near, far)
    returned = exchange(answers, "dom")
    forcing, surge = finish(place, need_tiles, returned, message, elevation, bed_level)
    return forcing.transpose(1, 0, 2), surge.reshape(1, -1)


def solution(mesh):
    placed = (
        P(("own", "dom"), None, None),
        P(),
        P(("own", "dom"), None),
        P(("own", "dom"), None),
        P(None, ("own", "dom"), None),
        P(("own", "dom")),
        P("own", "dom"),
        P("own", "dom"),
    )
    return jax.shard_map(
        shards,
        mesh=mesh,
        in_specs=placed,
        out_specs=(P(("own", "dom"), None, None), P("own", "dom")),
        check_vma=False,
    )
```

```python
import jax
import jax.numpy as jnp
from jax import lax
from jax.experimental import pallas as pl
from jax.experimental.pallas import tpu as pltpu
from jax.sharding import PartitionSpec as P

TILE = 64
TCOLS = 32
TILES_DEV = 2
FIELDS = 6
SWEEPS = 4
KAPPA = 0.08
NEED = 32
NPS = 1024
LANES = 128
GROUPS = NPS // LANES
N_OWN = 8
N_DOM = 64
BAND = TILES_DEV * N_DOM
CORES = 2
MSG = 16
CHUNK = 256
PER_CHUNK = CHUNK // LANES
CHUNKS = NPS // CHUNK
FIELD_BITS = 10
ABSENT = (CHUNKS - 1) * FIELD_BITS << 16
LIST = 8 * FIELD_BITS
DEAD_CELL = 0xFFC0
EDGE_SCALE = 2.0**29
FX_STEP = 2.0**-16
FY_TOP = 65535.0


SMALL = pltpu.CompilerParams(vmem_limit_bytes=8 * 2**20)


def iota(shape, dim):
    return lax.broadcasted_iota(jnp.int32, shape, dim)


def storm_field(place_ref, track_ref, background_ref, out_ref, rows_ref):
    field = iota((8, LANES), 0)
    lane = iota((8, LANES), 1)
    late = field >= 3
    centre_x, centre_y, deficit, max_radius, exponent = (
        jnp.where(late, track_ref[1, i], track_ref[0, i]) for i in range(5)
    )
    kind = jnp.where(late, field - 3, field)
    strength = exponent * deficit
    left = lane < TILE

    def one_field(tile, chunk):
        tile_index = place_ref[0] * TILES_DEV + tile
        north = (tile_index // TCOLS * TILE + 2 * chunk + lane // TILE).astype(jnp.float32)
        east = (tile_index % TCOLS * TILE + lane % TILE).astype(jnp.float32)
        offset_x = east - centre_x
        offset_y = north - centre_y
        radius = jnp.sqrt(offset_x * offset_x + offset_y * offset_y + 1.0)
        ratio = jnp.exp(exponent * jnp.log(max_radius / radius))
        decay = jnp.exp(-ratio)
        speed = jnp.sqrt(strength * ratio * decay)
        wind = speed * jnp.where(kind == 0, -offset_y, offset_x) / radius
        storm = jnp.where(kind == 2, -deficit * (1.0 - decay), wind)
        piece = background_ref[:, tile, pl.ds(pl.multiple_of(chunk * LANES, LANES), LANES)]
        return piece.astype(jnp.float32) + storm[:FIELDS]

    def step(chunk, carry):
        first = one_field(0, chunk)
        second = one_field(1, chunk)
        even = jnp.where(left[:FIELDS], first, pltpu.roll(second, TILE, 1))
        odd = jnp.where(left[:FIELDS], pltpu.roll(first, TILE, 1), second)
        rows_ref[pl.ds(2 * chunk, FIELDS, stride=TILE), :] = even
        rows_ref[pl.ds(2 * chunk + 1, FIELDS, stride=TILE), :] = odd
        return carry

    lax.fori_loop(0, TILE // 2, step, 0, unroll=8)
    out_ref[...] = rows_ref[0 : FIELDS * TILE, :].astype(jnp.bfloat16)


def column_code(fraction):
    scaled = fraction * 32768.0
    whole = jnp.floor(scaled)
    code = 2.0 * whole + jnp.where(scaled > whole, 1.0, 0.0)
    return jnp.minimum(code, 65535.0).astype(jnp.int32)


def row_code(fraction):
    return jnp.floor(fraction * FY_TOP + 0.5).astype(jnp.int32)


def edge_code(value):
    return jnp.floor(value * EDGE_SCALE + 0.5).astype(jnp.int32)


def prepare_kernel(
    place_ref,
    track_ref,
    need_ref,
    count_ref,
    background_ref,
    cells_ref,
    fracs_ref,
    ehead_ref,
    etail_ref,
    bhead_ref,
    btail_ref,
    tiles_ref,
    out_ref,
    rows_ref,
    stage_ref,
):
    storm_field(place_ref, track_ref, background_ref, tiles_ref, rows_ref)
    for g in range(GROUPS):
        span = slice(g * LANES, (g + 1) * LANES)
        word = cells_ref[:, span] | (column_code(fracs_ref[0, :, span]) << 16)
        stage_ref[pl.ds(g, NEED, stride=MSG), :] = word
    for g in range(GROUPS // 2):
        low = row_code(fracs_ref[1, :, g * LANES : (g + 1) * LANES])
        high = row_code(fracs_ref[1, :, NPS // 2 + g * LANES : NPS // 2 + (g + 1) * LANES])
        stage_ref[pl.ds(GROUPS + g, NEED, stride=MSG), :] = low | (high << 16)
    row = iota((8, LANES), 0)
    lane = iota((8, LANES), 1)
    position = row * LANES + lane
    surface = jnp.where(lane < SWEEPS, ehead_ref[0:1, :], etail_ref[7:8, :])
    bed = jnp.where(lane < SWEEPS, bhead_ref[0:1, :], btail_ref[7:8, :])
    plain = jnp.where(row == 5, edge_code(surface), jnp.where(row == 6, edge_code(bed), ABSENT))

    def clear(d, carry):
        out_ref[d, 8:16, :] = plain
        return carry

    lax.fori_loop(0, N_DOM, clear, 0, unroll=8)

    def place(s, carry):
        tile = need_ref[0, s]
        count = count_ref[s]
        holder = tile % BAND // TILES_DEV
        live = jnp.maximum((count + CHUNK - 1) // CHUNK, 2)
        header = (tile // BAND * TILES_DEV + tile % TILES_DEV) | ((live - 2) * FIELD_BITS << 16)
        start = pl.multiple_of(s * MSG, MSG)
        out_ref[holder, 0:8, :] = jnp.where(position < count, stage_ref[pl.ds(start, 8), :], DEAD_CELL)
        out_ref[holder, 8:16, :] = jnp.where(
            row < 4, stage_ref[pl.ds(start + 8, 8), :], jnp.where(row == 4, header, plain)
        )
        return carry

    lax.fori_loop(0, NEED, place, 0, unroll=4)


def prepare(place, storm_track, need_tiles, slot_count, background, node_cells, node_fracs, elevation, bed_level):
    last = elevation.shape[0] // 8 - 1
    head = pl.BlockSpec((8, LANES), lambda i: (0, 0))
    tail = pl.BlockSpec((8, LANES), lambda i: (last, 0))
    vmem = pl.BlockSpec(memory_space=pltpu.VMEM)
    rows = FIELDS * TILE
    return pl.pallas_call(
        prepare_kernel,
        grid=(1,),
        out_shape=(
            jax.ShapeDtypeStruct((rows, LANES), jnp.bfloat16),
            jax.ShapeDtypeStruct((N_DOM, MSG, LANES), jnp.int32),
        ),
        in_specs=[pl.BlockSpec(memory_space=pltpu.SMEM)] * 4 + [vmem] * 3 + [head, tail, head, tail],
        out_specs=(vmem, vmem),
        scratch_shapes=[
            pltpu.VMEM((8 * TILE, LANES), jnp.float32),
            pltpu.VMEM((NEED * MSG, LANES), jnp.int32),
        ],
    )(
        place,
        storm_track,
        need_tiles,
        slot_count,
        background.transpose(1, 0, 2),
        node_cells,
        node_fracs,
        elevation,
        elevation,
        bed_level,
        bed_level,
    )


SLOT_ROWS = FIELDS * GROUPS * 8
HALF = FIELDS // 2


def interpolate_kernel(
    place_ref,
    message_ref,
    near0,
    near1,
    near2,
    near3,
    far_ref,
    out_ref,
    tiles_ref,
    x_ref,
    y_ref,
    part_ref,
    list_ref,
    header_ref,
    sem,
):
    headers = pltpu.make_async_copy(message_ref.at[:, 12:13, :], header_ref, sem)
    headers.start()
    own = place_ref[0] // N_DOM

    def keep(band, pair):
        tiles_ref[2 * band] = pair
        tiles_ref[2 * band + 1] = pltpu.roll(pair, TILE, 1)

    for shift, ref in enumerate((near0, near1, near2, near3)):
        band = (own + N_OWN - CORES * shift) % N_OWN
        keep(band, ref[...])
        keep(band + 1 - 2 * (band % CORES), far_ref[shift])

    headers.wait()
    packed = jnp.int32(0)
    for s in range(N_DOM):
        shift = header_ref[s, 0, 0] >> 16
        list_ref[shift * 8 + (lax.shift_right_logical(packed, shift) & (2**FIELD_BITS - 1))] = s
        packed = packed + (1 << shift)
    counts = [packed >> i * FIELD_BITS & (2**FIELD_BITS - 1) for i in range(CHUNKS - 1)]
    spot = iota((TILE, LANES), 0).astype(jnp.float32)

    def add_up(i, slot):
        values = []
        for f in range(FIELDS):
            at = i * SLOT_ROWS + f * 64
            pieces = [part_ref[pl.ds(at + j, GROUPS, stride=8), :] for j in range(8)]
            while len(pieces) > 1:
                pieces = [a + b for a, b in zip(pieces[::2], pieces[1::2])]
            values.append(pieces[0])
        out_ref[slot] = jnp.concatenate(values, axis=0).astype(jnp.bfloat16)

    def hat(ref, at):
        return jnp.maximum(1.0 - jnp.abs(spot - ref[at : at + 1, :]), 0.0)

    def decode(i, s):
        word = message_ref[s, 0:8, :]
        pair = message_ref[s, 8:16, :]
        cell = word & 0xFFFF
        row = (cell // TILE).astype(jnp.float32)
        low = (pair[0:4] & 0xFFFF).astype(jnp.float32)
        high = lax.shift_right_logical(pair[0:4], 16).astype(jnp.float32)
        x_ref[8 * i : 8 * i + 8, :] = (cell & (TILE - 1)).astype(jnp.float32) + lax.shift_right_logical(
            word, 16
        ).astype(jnp.float32) * FX_STEP
        y_ref[8 * i : 8 * i + 4, :] = row[0:4] + low * (1.0 / FY_TOP)
        y_ref[8 * i + 4 : 8 * i + 8, :] = row[4:8] + high * (1.0 / FY_TOP)

    def two_slots(slots, before, live):
        for i in range(2):
            add_up(i, before[i])
        for i in range(2):
            decode(i, slots[i])
        tiles = [tiles_ref[header_ref[s, 0, 0] & 0xFFFF, :, 0:TILE] for s in slots]
        for c in range(live):
            for i in range(2):
                groups = range(c * PER_CHUNK, (c + 1) * PER_CHUNK)
                columns = jnp.concatenate([hat(x_ref, 8 * i + g).astype(jnp.bfloat16) for g in groups], axis=1)
                rows = jnp.concatenate([hat(y_ref, 8 * i + g) for g in groups], axis=1)
                for f in range(FIELDS):
                    if f % HALF == 0:
                        part = tiles[i][f * TILE : (f + HALF) * TILE]
                        spread = jnp.dot(part, columns, preferred_element_type=jnp.float32)
                    weighed = spread[f % HALF * TILE : (f % HALF + 1) * TILE] * rows
                    total = jnp.sum(weighed.reshape(TILE // 8, 8, CHUNK), axis=0)
                    for j, g in enumerate(groups):
                        at = i * SLOT_ROWS + (f * GROUPS + g) * 8
                        part_ref[at : at + 8, :] = total[:, j * LANES : (j + 1) * LANES]
        dead = (CHUNKS - live) * PER_CHUNK * 8
        if dead:
            for i in range(2):
                for f in range(FIELDS):
                    at = i * SLOT_ROWS + (f + 1) * GROUPS * 8 - dead
                    part_ref[at : at + dead, :] = jnp.zeros((dead, LANES), jnp.float32)

    before = (jnp.int32(-1), jnp.int32(-1))
    for i, n in enumerate(counts):

        @pl.when(n > 0)
        def _():
            list_ref[i * LIST + n] = list_ref[i * LIST + n - 1]

        def step(p, before):
            slots = (list_ref[i * LIST + 2 * p], list_ref[i * LIST + 2 * p + 1])
            two_slots(slots, tuple(jnp.where(b < 0, s, b) for b, s in zip(before, slots)), i + 2)
            return slots

        before = lax.fori_loop(0, (n + 1) // 2, step, before)
    for i in range(2):
        add_up(i, jnp.maximum(before[i], 0))


def interpolate(place, message, near, far):
    return pl.pallas_call(
        interpolate_kernel,
        out_shape=jax.ShapeDtypeStruct((N_DOM, FIELDS * GROUPS, LANES), jnp.bfloat16),
        in_specs=[pl.BlockSpec(memory_space=pltpu.SMEM)] + [pl.BlockSpec(memory_space=pltpu.VMEM)] * 6,
        out_specs=pl.BlockSpec(memory_space=pltpu.VMEM),
        scratch_shapes=[
            pltpu.VMEM((N_OWN * TILES_DEV, FIELDS * TILE, LANES), jnp.bfloat16),
            pltpu.VMEM((3 * GROUPS, LANES), jnp.float32),
            pltpu.VMEM((3 * GROUPS, LANES), jnp.float32),
            pltpu.VMEM((2 * SLOT_ROWS, LANES), jnp.float32),
            pltpu.SMEM((CHUNKS * LIST,), jnp.int32),
            pltpu.SMEM((N_DOM, 1, LANES), jnp.int32),
            pltpu.SemaphoreType.DMA,
        ],
        compiler_params=SMALL,
    )(place, message, *near, far)


def following(x, lane):
    moved = pltpu.roll(x, LANES - 1, 1)
    return jnp.where(lane == LANES - 1, pltpu.roll(moved, x.shape[0] - 1, 0), moved)


def preceding(x, lane):
    moved = pltpu.roll(x, 1, 1)
    return jnp.where(lane == 0, pltpu.roll(moved, 1, 0), moved)


def flux_sweeps(place_ref, before_ref, after_ref, elevation_ref, bed_ref, out_ref):
    rows = elevation_ref.shape[0]
    lane8 = iota((8, LANES), 1)
    row8 = iota((8, LANES), 0)

    def ends(which):
        before = before_ref[0, which : which + 1, :].astype(jnp.float32) * (1.0 / EDGE_SCALE)
        after = after_ref[0, which : which + 1, :].astype(jnp.float32) * (1.0 / EDGE_SCALE)
        top = jnp.where((row8 == 7) & (lane8 >= LANES - SWEEPS), before, 0.0)
        bottom = jnp.where((row8 == 0) & (lane8 < SWEEPS), after, 0.0)
        return top, bottom

    surface_top, surface_bottom = ends(5)
    bed_top, bed_bottom = ends(6)
    surface = jnp.concatenate([surface_top, elevation_ref[...], surface_bottom], axis=0)
    bed = jnp.concatenate([bed_top, bed_ref[...], bed_bottom], axis=0)
    lane = iota(surface.shape, 1)
    node = iota(surface.shape, 0) * LANES + lane
    dom = place_ref[0] % N_DOM
    first_wall = jnp.where(dom == 0, 8 * LANES - 1, -1)
    last_wall = jnp.where(dom == N_DOM - 1, (8 + rows) * LANES - 1, -1)
    open_face = jnp.where((node == first_wall) | (node == last_wall), 0.0, KAPPA)
    for _ in range(SWEEPS):
        wet = jnp.maximum(surface - bed, 0.0)
        drop = surface - following(surface, lane)
        upwind = jnp.where(drop >= 0.0, wet, following(wet, lane))
        flux = open_face * upwind * drop
        surface = surface - (flux - preceding(flux, lane))
    out_ref[...] = surface[8 : 8 + rows]


SLOTS8 = 8


def finish_kernel(
    place_ref,
    need_ref,
    returned_ref,
    before_ref,
    after_ref,
    elevation_ref,
    bed_ref,
    forcing_ref,
    surge_ref,
    surface_ref,
    stage_ref,
):
    rows = FIELDS * GROUPS
    flux_sweeps(place_ref, before_ref, after_ref, elevation_ref, bed_ref, surface_ref)

    def eight_slots(b, carry):
        for i in range(SLOTS8):
            s = b * SLOTS8 + i
            block = returned_ref[need_ref[0, s] % BAND // TILES_DEV].astype(jnp.float32)
            stage_ref[i * rows : (i + 1) * rows, :] = block
            here = pl.ds(pl.multiple_of(s * GROUPS, GROUPS), GROUPS)
            surface = surface_ref[here, :]
            wet = jnp.minimum(jnp.maximum(surface - bed_ref[here, :], 0.0), 1.0)
            surge_ref[here, :] = surface - 0.5 * block[rows - GROUPS :] * wet
        slots = pl.ds(pl.multiple_of(b * SLOTS8, SLOTS8), SLOTS8)
        for f in range(FIELDS):
            for g in range(GROUPS):
                piece = stage_ref[pl.ds(f * GROUPS + g, SLOTS8, stride=rows), :]
                forcing_ref[f, slots, g * LANES : (g + 1) * LANES] = piece.astype(jnp.bfloat16)
        return carry

    lax.fori_loop(0, NEED // SLOTS8, eight_slots, 0)


def finish(place, need_tiles, returned, message, elevation, bed_level):
    def whole(shape):
        return pl.BlockSpec(shape, lambda i, *refs: (0,) * len(shape))

    def neighbour(step):
        return pl.BlockSpec((1, 8, LANES), lambda i, place_ref, need_ref: ((place_ref[0] + step) % N_DOM, 1, 0))

    forcing = (FIELDS, NEED, NPS)
    return pl.pallas_call(
        finish_kernel,
        out_shape=(
            jax.ShapeDtypeStruct(forcing, jnp.bfloat16),
            jax.ShapeDtypeStruct(elevation.shape, jnp.float32),
        ),
        grid_spec=pltpu.PrefetchScalarGridSpec(
            num_scalar_prefetch=2,
            grid=(1,),
            in_specs=[
                whole(returned.shape),
                neighbour(N_DOM - 1),
                neighbour(1),
                whole(elevation.shape),
                whole(elevation.shape),
            ],
            out_specs=(whole(forcing), whole(elevation.shape)),
            scratch_shapes=[
                pltpu.VMEM(elevation.shape, jnp.float32),
                pltpu.VMEM((SLOTS8 * FIELDS * GROUPS, LANES), jnp.float32),
            ],
        ),
        compiler_params=SMALL,
    )(place, need_tiles, returned, message, message, elevation, bed_level)


def exchange(blocks, axis):
    return lax.all_to_all(blocks, axis, split_axis=0, concat_axis=0, tiled=True)


def shards(
    background, storm_track, need_tiles, node_cells, node_fracs, slot_count, elevation, bed_level
):
    place = (lax.axis_index("own") * N_DOM + lax.axis_index("dom"))[None].astype(jnp.int32)
    elevation = elevation.reshape(-1, LANES)
    bed_level = bed_level.reshape(-1, LANES)
    tiles, question = prepare(
        place, storm_track, need_tiles, slot_count, background, node_cells, node_fracs, elevation, bed_level
    )
    near = [tiles]
    for shift in range(CORES, N_OWN, CORES):
        near.append(lax.ppermute(tiles, "own", [(i, (i + shift) % N_OWN) for i in range(N_OWN)]))
    message = exchange(question, "dom")
    far = lax.ppermute(jnp.stack(near), "own", [(i, i ^ 1) for i in range(N_OWN)])
    answers = interpolate(place, message, near, far)
    returned = exchange(answers, "dom")
    forcing, surge = finish(place, need_tiles, returned, message, elevation, bed_level)
    return forcing.transpose(1, 0, 2), surge.reshape(1, -1)


def solution(mesh):
    placed = (
        P(("own", "dom"), None, None),
        P(),
        P(("own", "dom"), None),
        P(("own", "dom"), None),
        P(None, ("own", "dom"), None),
        P(("own", "dom")),
        P("own", "dom"),
        P("own", "dom"),
    )
    return jax.shard_map(
        shards,
        mesh=mesh,
        in_specs=placed,
        out_specs=(P(("own", "dom"), None, None), P("own", "dom")),
        check_vma=False,
    )
```
